32 devices in a mesh: dp: 8 (over z, x), expert: 4 (over y, core).
Axes of the slice: x: 2, y: 2, z: 4, core: 2. Of those that a mesh axis runs over, the one named last changes fastest.
Arguments:
- tokens: bfloat16 [4096, 2048], P(('dp', 'expert')), may hold values from -6 to 6
- out_grad: bfloat16 [4096, 2048], P(('dp', 'expert')), may hold values from -3 to 3
- z_weight: float32 [4096], P(('dp', 'expert')), may hold values from 0.1 to 1
- router_weight: bfloat16 [2048, 128], replicated, may hold values from -0.125 to 0.125
- expert_ids: int32 [4096, 4], P(('dp', 'expert')), may hold values from 0 to 127, as said below
- gate_up_weight: bfloat16 [4, 2048, 3072], P('expert'), may hold values from -0.125 to 0.125
- down_weight: bfloat16 [4, 1536, 2048], P('expert'), may hold values from -0.15625 to 0.15625
Outputs:
- token_grad: bfloat16 [4096, 2048], P(('dp', 'expert'))
- router_grad: float32 [2048, 128], replicated
- gate_up_grad: bfloat16 [4, 2048, 3072], P('expert', 'dp')
- down_grad: bfloat16 [4, 1536, 2048], P('expert', 'dp')
The draws below stay inside these ranges and needn't reach their ends.
Inputs may be any that keep to these rules, and one draw needn't show every extreme that they name: `expert_ids`: each row names 4 different experts. Experts 0 to 3 are the ones in flight. The 128 rows of one device name any one expert in flight at most 64 times; in every data group some expert in flight is named exactly 64 times by the rows of each device of the group.
All inputs are finite; a program needn't handle non-finite values.
Results may differ from the reference program's by a relative error of at most 0.019.
Values may be sent and summed in bfloat16 or wider, within the bound.
A program may use at most 192 MiB of HBM per device.

```python
import math
import jax
import jax.numpy as jnp
from jax import lax

D = 2048
FF = 1536
ROUTED = 128
TOP = 4
BLOCK = 128
TOK_DEV = 128
CAP = 64
FLIGHT = 4
TOKENS = 4096
N_DP = 8
N_EXPERT = 4


def draw_expert_ids(key, part):
    devices_all = TOKENS // TOK_DEV
    flight = N_EXPERT
    key_base, key_mask, key_hot, key_dev = jax.random.split(key, 4)
    base = jax.random.randint(key_base, (devices_all, flight), 0, CAP + 1)
    base = base * jax.random.randint(key_mask, (devices_all, flight), 0, 2)
    hot = jax.random.randint(key_hot, (devices_all // N_EXPERT,), 0, flight)
    hot_dev = jnp.repeat(hot, N_EXPERT)
    counts = jnp.where(jnp.arange(flight)[None, :] == hot_dev[:, None], CAP, base).astype(jnp.int32)
    others = ROUTED - flight
    spacing = others // TOP

    def one_device(count_row, dev_key):
        key_fill, key_order, key_perm = jax.random.split(dev_key, 3)
        ends = jnp.cumsum(count_row)
        total = ends[-1]
        demand = jnp.arange(TOP * TOK_DEV, dtype=jnp.int32)
        owner = jnp.sum((ends[None, :] <= demand[:, None]).astype(jnp.int32), axis=1)
        table = jnp.where(demand < total, owner, -1).reshape(TOP, TOK_DEV).T
        offset = jax.random.randint(key_fill, (TOK_DEV, 1), 0, others)
        fill = flight + (offset + jnp.arange(TOP, dtype=jnp.int32)[None, :] * spacing) % others
        table = jnp.where(table >= 0, table, fill)
        order_keys = jax.random.randint(key_order, (TOK_DEV, TOP), 0, 1 << 20) * TOP + jnp.arange(TOP, dtype=jnp.int32)[None, :]
        order = jnp.argsort(order_keys, axis=1, stable=True)
        table = jnp.take_along_axis(table, order, axis=1)
        shuffle = jax.random.permutation(key_perm, TOK_DEV)
        return table[shuffle]
    dev_keys = jax.random.split(key_dev, devices_all)
    result = jax.vmap(one_device)(counts, dev_keys)
    return result.reshape(TOKENS, TOP).astype(jnp.int32)


def block_levels(rng, dims, cuts, smallest, high):
    level = 1.0
    for position, shards_of in cuts:
        heights = jax.random.uniform(jax.random.fold_in(jax.random.fold_in(rng, 6), position), (shards_of,), jnp.float32, smallest / len(cuts), high / len(cuts))
        level = level * jnp.repeat(jnp.exp(heights), dims[position] // shards_of).reshape((-1,) + (1,) * (len(dims) - 1 - position))
    return level


def normal_values(rng, extent, scale, limit, shards=(), kind=jnp.bfloat16):
    entries = scale * jax.random.normal(rng, extent, jnp.float32)
    if shards:
        entries = entries * block_levels(rng, extent, shards, -0.22, 0.18)
    return jnp.clip(entries, -limit, limit).astype(kind)


def setup_inputs(seed: int = 0) -> dict:
    key_list = jax.random.split(jax.random.key(seed), 8)
    tokens = normal_values(key_list[0], (TOKENS, D), 1.0, 6.0, ((0, 32),))
    out_grad = normal_values(key_list[1], (TOKENS, D), 0.5, 3.0, ((0, 32),))
    z_weight = jnp.clip(jnp.exp(math.log(1.0) - 2.3025851 * jax.random.uniform(key_list[2], (TOKENS,), jnp.float32) ** block_levels(key_list[2], (TOKENS,), ((0, 32),), -0.2, 0.2)), 0.1, 1.0)
    router_weight = normal_values(key_list[3], (D, ROUTED), D ** -0.5, 0.125)
    expert_ids = draw_expert_ids(jax.random.fold_in(key_list[7], 71), 0)
    gate_up_weight = normal_values(key_list[5], (FLIGHT, D, 2 * FF), D ** -0.5, 0.125, ((0, 4),))
    down_weight = normal_values(key_list[6], (FLIGHT, FF, D), FF ** -0.5, 0.15625, ((0, 4),))
    return dict(tokens=tokens, out_grad=out_grad, z_weight=z_weight, router_weight=router_weight, expert_ids=expert_ids, gate_up_weight=gate_up_weight, down_weight=down_weight)


def expert_rows(rows_in, rows_grad, w_gateup, w_down, acc_gateup, acc_down):
    hidden_units = w_down.shape[0]
    pre_act = jnp.dot(rows_in, w_gateup, preferred_element_type=jnp.float32)
    gate_pre = pre_act[:, :hidden_units]
    up_pre = pre_act[:, hidden_units:]
    activated = jax.nn.silu(gate_pre)
    hidden = (activated * up_pre).astype(jnp.bfloat16)
    expert_out = jnp.dot(hidden, w_down, preferred_element_type=jnp.float32).astype(jnp.bfloat16)
    hidden_grad = lax.dot_general(rows_grad, w_down, (((1,), (1,)), ((), ())), preferred_element_type=jnp.float32)
    acc_down = acc_down + lax.dot_general(hidden, rows_grad, (((0,), (0,)), ((), ())), preferred_element_type=jnp.float32)
    sigmoid_gate = jax.nn.sigmoid(gate_pre)
    gate_grad = hidden_grad * up_pre * sigmoid_gate * (1.0 + gate_pre * (1.0 - sigmoid_gate))
    up_grad = hidden_grad * activated
    pre_grad = jnp.concatenate([gate_grad, up_grad], axis=1).astype(jnp.bfloat16)
    acc_gateup = acc_gateup + lax.dot_general(rows_in, pre_grad, (((0,), (0,)), ((), ())), preferred_element_type=jnp.float32)
    input_grad = lax.dot_general(pre_grad, w_gateup, (((1,), (1,)), ((), ())), preferred_element_type=jnp.float32).astype(jnp.bfloat16)
    return acc_gateup, acc_down, expert_out, input_grad


def run_blocks(work_in, work_grad, w_gateup, w_down, nblocks):
    width = work_in.shape[1]
    hidden_units = w_down.shape[0]
    start_state = (jnp.zeros((width, 2 * hidden_units), jnp.float32), jnp.zeros((hidden_units, width), jnp.float32),
                   jnp.zeros_like(work_in), jnp.zeros_like(work_in))

    def step(block_index, carry):
        acc_gateup, acc_down, out_rows, grad_rows = carry
        start = (block_index * BLOCK).astype(jnp.int32)
        rows_in = lax.dynamic_slice_in_dim(work_in, start, BLOCK, 0)
        rows_grad = lax.dynamic_slice_in_dim(work_grad, start, BLOCK, 0)
        acc_gateup, acc_down, produced, backward = expert_rows(rows_in, rows_grad, w_gateup, w_down, acc_gateup, acc_down)
        out_rows = lax.dynamic_update_slice_in_dim(out_rows, produced, start, 0)
        grad_rows = lax.dynamic_update_slice_in_dim(grad_rows, backward, start, 0)
        return acc_gateup, acc_down, out_rows, grad_rows

    return lax.fori_loop(jnp.int32(0), nblocks.astype(jnp.int32), step, start_state)


def reference(tokens, out_grad, z_weight, router_weight, expert_ids, gate_up_weight, down_weight):
    logits = jnp.dot(tokens, router_weight, preferred_element_type=jnp.float32)
    choose = expert_ids[:, :, None] == jnp.arange(ROUTED, dtype=jnp.int32)[None, None, :]
    selected = jnp.sum(jnp.where(choose, logits[:, None, :], 0.0), axis=2)
    sel_exp = jnp.exp(selected)
    probs = sel_exp / jnp.sum(sel_exp, axis=1, keepdims=True)
    log_total = jnp.log(jnp.sum(jnp.exp(logits), axis=1))
    slots_group = N_EXPERT * TOK_DEV * TOP
    rows_max = N_EXPERT * CAP
    group_ids = expert_ids.reshape(N_DP, slots_group)
    group_prob = probs.reshape(N_DP, slots_group)
    group_tok = tokens.reshape(N_DP, N_EXPERT * TOK_DEV, D)
    group_grad = out_grad.reshape(N_DP, N_EXPERT * TOK_DEV, D)

    def one_group(carry, data):
        ids_here, prob_here, tok_here, grad_here = data

        def one_expert(expert):
            member = ids_here == expert
            rank = jnp.cumsum(member.astype(jnp.int32)) - 1
            place = jnp.where(member, rank, rows_max).astype(jnp.int32)
            source = jnp.zeros((rows_max,), jnp.int32).at[place].set(jnp.arange(slots_group, dtype=jnp.int32), mode="drop")
            valid = jnp.zeros((rows_max,), jnp.bool_).at[place].set(True, mode="drop")
            tok_index = source // TOP
            rows_in = jnp.where(valid[:, None], tok_here[tok_index], 0)
            rows_grad = jnp.where(valid[:, None], prob_here[source][:, None] * grad_here[tok_index].astype(jnp.float32), 0.0).astype(jnp.bfloat16)
            used = (jnp.sum(member.astype(jnp.int32)) + BLOCK - 1) // BLOCK
            acc_gateup, acc_down, produced, backward = run_blocks(rows_in, rows_grad, gate_up_weight[expert], down_weight[expert], used)
            return acc_gateup.astype(jnp.bfloat16), acc_down.astype(jnp.bfloat16), produced, backward, source, valid

        part_gu, part_down, outs, backs, sources, valids = lax.map(one_expert, jnp.arange(N_EXPERT, dtype=jnp.int32))
        sum_gu, sum_down = carry
        sum_gu = sum_gu + part_gu.astype(jnp.float32)
        sum_down = sum_down + part_down.astype(jnp.float32)
        target = jnp.where(valids.reshape(-1), sources.reshape(-1), slots_group).astype(jnp.int32)
        slot_out = jnp.zeros((slots_group, D), jnp.bfloat16).at[target].set(outs.reshape(-1, D), mode="drop")
        slot_back = jnp.zeros((slots_group, D), jnp.bfloat16).at[target].set(backs.reshape(-1, D), mode="drop")
        return (sum_gu, sum_down), (slot_out, slot_back)

    start_sums = (jnp.zeros((N_EXPERT, D, 2 * FF), jnp.float32), jnp.zeros((N_EXPERT, FF, D), jnp.float32))
    (sum_gu, sum_down), (slot_out, slot_back) = lax.scan(one_group, start_sums, (group_ids, group_prob, group_tok, group_grad))
    slot_out = slot_out.reshape(TOKENS, TOP, D)
    slot_back = slot_back.reshape(TOKENS, TOP, D)
    scores = jnp.sum(out_grad[:, None, :].astype(jnp.float32) * slot_out.astype(jnp.float32), axis=2)
    mean_score = jnp.sum(probs * scores, axis=1, keepdims=True)
    sel_grad = probs * (scores - mean_score)
    z_grad = 2.0 * z_weight[:, None] * log_total[:, None] * jnp.exp(logits - log_total[:, None])
    logit_grad = (z_grad + jnp.sum(jnp.where(choose, sel_grad[:, :, None], 0.0), axis=1)).astype(jnp.bfloat16)
    token_grad = (jnp.sum(slot_back.astype(jnp.float32), axis=1)
                  + lax.dot_general(logit_grad, router_weight, (((1,), (1,)), ((), ())), preferred_element_type=jnp.float32)).astype(jnp.bfloat16)
    router_grad = lax.dot_general(tokens, logit_grad, (((0,), (0,)), ((), ())), preferred_element_type=jnp.float32)
    return token_grad, router_grad, sum_gu.astype(jnp.bfloat16), sum_down.astype(jnp.bfloat16)
```

```python
import functools

import jax
import jax.numpy as jnp
from jax import lax
from jax.experimental import pallas as pl
from jax.experimental.pallas import tpu as pltpu
from jax.sharding import PartitionSpec as P

F32 = jnp.float32
BF16 = jnp.bfloat16
MESH = pl.DeviceIdType.MESH


def ring_order(count):
    inner = max(k for k in range(1, count + 1) if count % k == 0 and k * k <= count)
    outer = count // inner
    if inner == 1 or outer % 2:
        return list(range(count))
    order = []
    for row in range(outer):
        cols = list(range(1, inner))
        order += [row * inner + col for col in (cols if row % 2 == 0 else cols[::-1])]
    return order + [row * inner for row in range(outer)][::-1]


def lookup(table, key):
    value = jnp.int32(0)
    for slot, entry in enumerate(table):
        value = value + jnp.where(key == slot, jnp.int32(entry), jnp.int32(0))
    return value


def grads_kernel(
    copies, flight, order,
    xt_ref, pg_ref, ht_ref, dy_ref, rp_ref,
    gu_ref, dn_ref, rout_ref,
    gu_buf, dn_buf, rx_e, rsum, rx_d, rfull,
    send_sem, recv_sem, es_send, es_recv, ds_send, ds_recv, dg_send, dg_recv, eg_send, eg_recv,
):
    d = lax.axis_index("dp")
    e = lax.axis_index("expert")
    n = copies
    place = [order.index(i) for i in range(n)]
    pos = lookup(place, d)
    right = lookup(order, lax.rem(pos + 1, n))
    left = lookup(order, lax.rem(pos + n - 1, n))
    towards = (right, left)

    barrier = pltpu.get_barrier_semaphore()
    for k in range(1, n):
        pl.semaphore_signal(barrier, inc=1, device_id=(lax.rem(d + k, n), e), device_id_type=MESH)
    for k in range(1, flight):
        pl.semaphore_signal(barrier, inc=1, device_id=(d, lax.rem(e + k, flight)), device_id_type=MESH)
    pl.semaphore_wait(barrier, n + flight - 2)

    gu_rows = gu_ref.shape[1]
    half_rows = gu_rows // 2
    dn_rows = dn_ref.shape[1]
    gu_cols = gu_ref.shape[2] // 2
    dn_cols = dn_ref.shape[2] // 2
    piece_e = rsum.shape[0]
    piece_d = rx_d.shape[1]

    def owner_at(way, step):
        if way == 0:
            return lookup(order, lax.rem(pos + 2 * n - 1 - step, n))
        return lookup(order, lax.rem(pos + 1 + step, n))

    def own(way, part, owner):
        if part < 2:
            start = pl.multiple_of(owner * gu_rows + part * half_rows, half_rows)
            return jnp.dot(
                xt_ref[pl.ds(start, half_rows), :],
                pg_ref[:, way * gu_cols:(way + 1) * gu_cols],
                preferred_element_type=F32,
            )
        start = pl.multiple_of(owner * dn_rows, dn_rows)
        return jnp.dot(
            ht_ref[pl.ds(start, dn_rows), :],
            dy_ref[:, way * dn_cols:(way + 1) * dn_cols],
            preferred_element_type=F32,
        )

    def slot(way, part, step):
        return gu_buf.at[way, part, step] if part < 2 else dn_buf.at[way, step]

    def hop(way, part, step):
        return pltpu.make_async_remote_copy(
            src_ref=slot(way, part, step),
            dst_ref=slot(way, part, step + 1),
            send_sem=send_sem.at[way, part, step],
            recv_sem=recv_sem.at[way, part, step],
            device_id=(towards[way], e),
            device_id_type=MESH,
        )

    def share_e(k):
        to = lax.rem(e + k, flight)
        return pltpu.make_async_remote_copy(
            src_ref=rp_ref.at[pl.ds(pl.multiple_of(to * piece_e, piece_e), piece_e), :],
            dst_ref=rx_e.at[k - 1],
            send_sem=es_send.at[k - 1], recv_sem=es_recv.at[k - 1],
            device_id=(d, to), device_id_type=MESH,
        )

    def share_d(k):
        to = lax.rem(d + k, n)
        return pltpu.make_async_remote_copy(
            src_ref=rsum.at[pl.ds(pl.multiple_of(to * piece_d, piece_d), piece_d), :],
            dst_ref=rx_d.at[k - 1],
            send_sem=ds_send.at[k - 1], recv_sem=ds_recv.at[k - 1],
            device_id=(to, e), device_id_type=MESH,
        )

    def gather_d(k, source):
        rows = pl.ds(pl.multiple_of(e * piece_e + source * piece_d, piece_d), piece_d)
        return pltpu.make_async_remote_copy(
            src_ref=rfull.at[rows, :], dst_ref=rfull.at[rows, :],
            send_sem=dg_send.at[k - 1], recv_sem=dg_recv.at[k - 1],
            device_id=(lax.rem(d + k, n), e), device_id_type=MESH,
        )

    def gather_e(k, source):
        rows = pl.ds(pl.multiple_of(source * piece_e, piece_e), piece_e)
        return pltpu.make_async_remote_copy(
            src_ref=rfull.at[rows, :], dst_ref=rfull.at[rows, :],
            send_sem=eg_send.at[k - 1], recv_sem=eg_recv.at[k - 1],
            device_id=(d, lax.rem(e + k, flight)), device_id_type=MESH,
        )

    for part in range(3):
        for way in range(2):
            slot(way, part, 0)[...] = own(way, part, owner_at(way, 0)).astype(BF16)
            hop(way, part, 0).start()
    for k in range(1, flight):
        share_e(k).start()

    def middle(step, carry):
        for part in range(3):
            for way in range(2):
                hop(way, part, step - 1).wait_recv()
                here = slot(way, part, step)
                here[...] = (
                    here[...].astype(F32) + own(way, part, owner_at(way, step))
                ).astype(BF16)
                hop(way, part, step).start()

        @pl.when(step == 1)
        def _():
            total = rp_ref[pl.ds(pl.multiple_of(e * piece_e, piece_e), piece_e), :]
            for k in range(1, flight):
                share_e(k).wait_recv()
                total = total + rx_e[k - 1]
            rsum[...] = total
            for k in range(1, n):
                share_d(k).start()

        @pl.when(step == 2)
        def _():
            total = rsum[pl.ds(pl.multiple_of(d * piece_d, piece_d), piece_d), :]
            for k in range(1, n):
                share_d(k).wait_recv()
                total = total + rx_d[k - 1]
            rfull[pl.ds(pl.multiple_of(e * piece_e + d * piece_d, piece_d), piece_d), :] = total
            for k in range(1, n):
                gather_d(k, d).start()

        @pl.when(step == 3)
        def _():
            for k in range(1, n):
                gather_d(k, lax.rem(d + n - k, n)).wait_recv()
            for k in range(1, flight):
                gather_e(k, e).start()

        return carry

    lax.fori_loop(1, n - 1, middle, 0)

    for k in range(1, flight):
        gather_e(k, lax.rem(e + flight - k, flight)).wait_recv()
    rout_ref[...] = rfull[...]
    for part in range(3):
        for way in range(2):
            hop(way, part, n - 2).wait_recv()
            total = slot(way, part, n - 1)[...].astype(F32) + own(way, part, d)
            if part < 2:
                gu_ref[
                    0, part * half_rows:(part + 1) * half_rows, way * gu_cols:(way + 1) * gu_cols
                ] = total.astype(BF16)
            else:
                dn_ref[0, :, way * dn_cols:(way + 1) * dn_cols] = total.astype(BF16)

    def drain(step, carry):
        for part in range(3):
            for way in range(2):
                hop(way, part, step).wait_send()
        return carry

    lax.fori_loop(0, n - 1, drain, 0)
    for k in range(1, n):
        share_d(k).wait_send()
        gather_d(k, d).wait_send()
    for k in range(1, flight):
        share_e(k).wait_send()
        gather_e(k, e).wait_send()


def reduce_grads(copies, flight, xt, pre_grad, ht, dyk, router_part):
    width, rows = xt.shape
    gate_up = pre_grad.shape[1]
    hidden = ht.shape[0]
    routed = router_part.shape[1]
    n = copies
    gu_rows, dn_rows = width // n, hidden // n
    piece_e = width // flight
    piece_d = piece_e // n
    dma = pltpu.SemaphoreType.DMA
    vmem = pl.BlockSpec(memory_space=pltpu.VMEM)
    return pl.pallas_call(
        functools.partial(grads_kernel, n, flight, ring_order(n)),
        out_shape=(
            jax.ShapeDtypeStruct((1, gu_rows, gate_up), BF16),
            jax.ShapeDtypeStruct((1, dn_rows, width), BF16),
            jax.ShapeDtypeStruct((width, routed), F32),
        ),
        in_specs=[vmem] * 5,
        out_specs=(vmem,) * 3,
        scratch_shapes=[
            pltpu.VMEM((2, 2, n, gu_rows // 2, gate_up // 2), BF16),
            pltpu.VMEM((2, n, dn_rows, width // 2), BF16),
            pltpu.VMEM((flight - 1, piece_e, routed), F32),
            pltpu.VMEM((piece_e, routed), F32),
            pltpu.VMEM((n - 1, piece_d, routed), F32),
            pltpu.VMEM((width, routed), F32),
            dma((2, 3, n - 1)), dma((2, 3, n - 1)),
            dma((flight - 1,)), dma((flight - 1,)),
            dma((n - 1,)), dma((n - 1,)),
            dma((n - 1,)), dma((n - 1,)),
            dma((flight - 1,)), dma((flight - 1,)),
        ],
        compiler_params=pltpu.CompilerParams(
            collective_id=0, has_side_effects=True, vmem_limit_bytes=50 * 2**20
        ),
        cost_estimate=pl.CostEstimate(
            flops=2 * rows * width * (gate_up + hidden),
            bytes_accessed=2 * (width * gate_up + hidden * width) // n,
            transcendentals=0,
        ),
        name="grads",
    )(xt, pre_grad, ht, dyk, router_part)

def expert_rows(rows_in, rows_grad, w_gateup, w_down):
    hidden_units = w_down.shape[0]
    pre_act = jnp.dot(rows_in, w_gateup, preferred_element_type=F32)
    gate_pre = pre_act[:, :hidden_units]
    up_pre = pre_act[:, hidden_units:]
    activated = jax.nn.silu(gate_pre)
    hidden = (activated * up_pre).astype(BF16)
    expert_out = jnp.dot(hidden, w_down, preferred_element_type=F32).astype(BF16)
    hidden_grad = lax.dot_general(
        rows_grad, w_down, (((1,), (1,)), ((), ())), preferred_element_type=F32
    )
    sigmoid_gate = jax.nn.sigmoid(gate_pre)
    gate_grad = hidden_grad * up_pre * sigmoid_gate * (1.0 + gate_pre * (1.0 - sigmoid_gate))
    up_grad = hidden_grad * activated
    pre_grad = jnp.concatenate([gate_grad, up_grad], axis=1).astype(BF16)
    input_grad = lax.dot_general(
        pre_grad, w_gateup, (((1,), (1,)), ((), ())), preferred_element_type=F32
    ).astype(BF16)
    return (hidden, pre_grad, expert_out, input_grad)


def split_pair(values):
    upper = values.astype(jnp.bfloat16)
    lower = (values - upper.astype(jnp.float32)).astype(jnp.bfloat16)
    return jnp.stack([upper, lower], axis=-1)


def join_pair(pair):
    return pair[..., 0].astype(jnp.float32) + pair[..., 1].astype(jnp.float32)


def per_device(tokens, out_grad, z_weight, router_weight, expert_ids, gate_up_weight, down_weight):
    tok_count, width = tokens.shape
    top_count = expert_ids.shape[1]
    routed = router_weight.shape[1]
    flight = lax.axis_size("expert")
    capacity = tok_count // 2
    w_gateup = gate_up_weight[0]
    w_down = down_weight[0]
    hidden_units = w_down.shape[0]
    logits = jnp.dot(tokens, router_weight, preferred_element_type=jnp.float32)
    choose = expert_ids[:, :, None] == jnp.arange(routed, dtype=jnp.int32)[None, None, :]
    selected = jnp.sum(jnp.where(choose, logits[:, None, :], 0.0), axis=2)
    sel_exp = jnp.exp(selected)
    probs = sel_exp / jnp.sum(sel_exp, axis=1, keepdims=True)
    log_total = jnp.log(jnp.sum(jnp.exp(logits), axis=1))
    flat_ids = expert_ids.reshape(-1)
    slot_count = tok_count * top_count
    member = (flat_ids[:, None] == jnp.arange(flight, dtype=jnp.int32)[None, :]).astype(jnp.int32)
    ranks = jnp.sum((jnp.cumsum(member, axis=0) - 1) * member, axis=1)
    in_flight = flat_ids < flight
    position = jnp.where(in_flight, flat_ids * capacity + ranks, flight * capacity)
    source_slot = (
        jnp.zeros((flight * capacity,), jnp.int32)
        .at[position]
        .set(jnp.arange(slot_count, dtype=jnp.int32), mode="drop")
    )
    filled = jnp.zeros((flight * capacity,), jnp.bool_).at[position].set(True, mode="drop")
    source_tok = source_slot // top_count
    send_in = jnp.where(filled[:, None], tokens[source_tok], 0)
    slot_prob = jnp.where(filled, probs.reshape(-1)[source_slot], 0.0)
    counts = jnp.sum(member, axis=0)
    count_msg = jnp.stack([counts // 128, counts % 128], axis=1).astype(jnp.bfloat16)
    send_raw = jnp.where(filled[:, None], out_grad[source_tok], 0)
    prob_pair = split_pair(slot_prob)
    recv_in, recv_raw, recv_prob, recv_counts = (
        lax.all_to_all(
            send_in.reshape(flight, capacity, width),
            "expert",
            split_axis=0,
            concat_axis=0,
            tiled=True,
        ),
        lax.all_to_all(
            send_raw.reshape(flight, capacity, width),
            "expert",
            split_axis=0,
            concat_axis=0,
            tiled=True,
        ),
        lax.all_to_all(
            prob_pair.reshape(flight, capacity, 2),
            "expert",
            split_axis=0,
            concat_axis=0,
            tiled=True,
        ),
        lax.all_to_all(count_msg, "expert", split_axis=0, concat_axis=0, tiled=True),
    )
    sources = recv_in.shape[0]
    total_rows = sources * capacity
    flat_in = recv_in.reshape(total_rows, width)
    flat_raw = recv_raw.reshape(total_rows, width)
    row_prob = join_pair(recv_prob.reshape(total_rows, 2))
    flat_grad = (row_prob[:, None] * flat_raw.astype(jnp.float32)).astype(jnp.bfloat16)
    hidden, pre_grad, produced, back_rows = expert_rows(flat_in, flat_grad, w_gateup, w_down)
    slot_at = jnp.where(in_flight, position, 0)
    row_score = jnp.sum(flat_raw.astype(jnp.float32) * produced.astype(jnp.float32), axis=1)
    score_pair = split_pair(row_score)
    home_dx, home_pair = (
        lax.all_to_all(
            back_rows.reshape(sources, capacity, width),
            "expert",
            split_axis=0,
            concat_axis=0,
            tiled=True,
        ),
        lax.all_to_all(
            score_pair.reshape(sources, capacity, 2),
            "expert",
            split_axis=0,
            concat_axis=0,
            tiled=True,
        ),
    )
    flat_dx = home_dx.reshape(flight * capacity, width)
    flat_score = join_pair(home_pair.reshape(flight * capacity, 2))
    scores = jnp.where(in_flight, flat_score[slot_at], 0.0).reshape(tok_count, top_count)
    slot_dx = jnp.where(in_flight[:, None], flat_dx[slot_at], 0).reshape(
        tok_count, top_count, width
    )
    mean_score = jnp.sum(probs * scores, axis=1, keepdims=True)
    sel_grad = probs * (scores - mean_score)
    z_grad = 2.0 * z_weight[:, None] * log_total[:, None] * jnp.exp(logits - log_total[:, None])
    logit_grad = (z_grad + jnp.sum(jnp.where(choose, sel_grad[:, :, None], 0.0), axis=1)).astype(
        jnp.bfloat16
    )
    token_grad = (
        jnp.sum(slot_dx.astype(jnp.float32), axis=1)
        + lax.dot_general(
            logit_grad, router_weight, (((1,), (1,)), ((), ())), preferred_element_type=jnp.float32
        )
    ).astype(jnp.bfloat16)
    router_part = lax.dot_general(
        tokens, logit_grad, (((0,), (0,)), ((), ())), preferred_element_type=jnp.float32
    )
    gate_up_grad, down_grad, router_grad = reduce_grads(
        lax.axis_size("dp"), flight, flat_in.T, pre_grad, hidden.T, flat_grad, router_part
    )
    return (token_grad, router_grad, gate_up_grad, down_grad)


def solution(mesh):
    return jax.shard_map(
        per_device,
        mesh=mesh,
        in_specs=(
            P(("dp", "expert"), None),
            P(("dp", "expert"), None),
            P(("dp", "expert")),
            P(),
            P(("dp", "expert"), None),
            P("expert", None, None),
            P("expert", None, None),
        ),
        out_specs=(
            P(("dp", "expert"), None),
            P(),
            P("expert", "dp", None),
            P("expert", "dp", None),
        ),
        check_vma=False,
    )
```

```python
import functools

import jax
import jax.numpy as jnp
from jax import lax
from jax.experimental import pallas as pl
from jax.experimental.pallas import tpu as pltpu
from jax.sharding import PartitionSpec as P

F32 = jnp.float32
BF16 = jnp.bfloat16
MESH = pl.DeviceIdType.MESH


def ring_order(count):
    inner = max(k for k in range(1, count + 1) if count % k == 0 and k * k <= count)
    outer = count // inner
    if inner == 1 or outer % 2:
        return list(range(count))
    order = []
    for row in range(outer):
        cols = list(range(1, inner))
        order += [row * inner + col for col in (cols if row % 2 == 0 else cols[::-1])]
    return order + [row * inner for row in range(outer)][::-1]


def lookup(table, key):
    value = jnp.int32(0)
    for slot, entry in enumerate(table):
        value = value + jnp.where(key == slot, jnp.int32(entry), jnp.int32(0))
    return value


def grads_kernel(
    copies, flight, order,
    xt_ref, pg_ref, ht_ref, dy_ref, score_ref, wg_hbm, tokt_ref, rw_ref, logit_ref, small_ref, ids_ref,
    gu_ref, dn_ref, rout_ref, tg_ref,
    gu_buf, dn_buf, rx_e, rsum, rx_d, rfull, rp_ref, wg_ref, back, home_dx, home_score, lg_ref,
    send_sem, recv_sem, es_send, es_recv, ds_send, ds_recv, dg_send, dg_recv, eg_send, eg_recv,
    wg_sem, dx_send, dx_recv, sc_send, sc_recv,
):
    d = lax.axis_index("dp")
    e = lax.axis_index("expert")
    n = copies
    place = [order.index(i) for i in range(n)]
    pos = lookup(place, d)
    right = lookup(order, lax.rem(pos + 1, n))
    left = lookup(order, lax.rem(pos + n - 1, n))
    towards = (right, left)

    load_w = pltpu.make_async_copy(wg_hbm, wg_ref, wg_sem)
    load_w.start()
    barrier = pltpu.get_barrier_semaphore()
    for k in range(1, n):
        pl.semaphore_signal(barrier, inc=1, device_id=(lax.rem(d + k, n), e), device_id_type=MESH)
    for k in range(1, flight):
        pl.semaphore_signal(barrier, inc=1, device_id=(d, lax.rem(e + k, flight)), device_id_type=MESH)
    pl.semaphore_wait(barrier, n + flight - 2)

    gu_rows = gu_ref.shape[1]
    half_rows = gu_rows // 2
    dn_rows = dn_ref.shape[1]
    gu_cols = gu_ref.shape[2] // 2
    dn_cols = dn_ref.shape[2] // 2
    piece_e = rsum.shape[0]
    piece_d = rx_d.shape[1]

    def owner_at(way, step):
        if way == 0:
            return lookup(order, lax.rem(pos + 2 * n - 1 - step, n))
        return lookup(order, lax.rem(pos + 1 + step, n))

    def own(way, part, owner):
        if part < 2:
            start = pl.multiple_of(owner * gu_rows + part * half_rows, half_rows)
            return jnp.dot(
                xt_ref[pl.ds(start, half_rows), :],
                pg_ref[:, way * gu_cols:(way + 1) * gu_cols],
                preferred_element_type=F32,
            )
        start = pl.multiple_of(owner * dn_rows, dn_rows)
        return jnp.dot(
            ht_ref[pl.ds(start, dn_rows), :],
            dy_ref[:, way * dn_cols:(way + 1) * dn_cols],
            preferred_element_type=F32,
        )

    def slot(way, part, step):
        return gu_buf.at[way, part, step] if part < 2 else dn_buf.at[way, step]

    def hop(way, part, step):
        return pltpu.make_async_remote_copy(
            src_ref=slot(way, part, step),
            dst_ref=slot(way, part, step + 1),
            send_sem=send_sem.at[way, part, step],
            recv_sem=recv_sem.at[way, part, step],
            device_id=(towards[way], e),
            device_id_type=MESH,
        )

    def share_e(k):
        to = lax.rem(e + k, flight)
        return pltpu.make_async_remote_copy(
            src_ref=rp_ref.at[pl.ds(pl.multiple_of(to * piece_e, piece_e), piece_e), :],
            dst_ref=rx_e.at[k - 1],
            send_sem=es_send.at[k - 1], recv_sem=es_recv.at[k - 1],
            device_id=(d, to), device_id_type=MESH,
        )

    def share_d(k):
        to = lax.rem(d + k, n)
        return pltpu.make_async_remote_copy(
            src_ref=rsum.at[pl.ds(pl.multiple_of(to * piece_d, piece_d), piece_d), :],
            dst_ref=rx_d.at[k - 1],
            send_sem=ds_send.at[k - 1], recv_sem=ds_recv.at[k - 1],
            device_id=(to, e), device_id_type=MESH,
        )

    def gather_d(k, source):
        rows = pl.ds(pl.multiple_of(e * piece_e + source * piece_d, piece_d), piece_d)
        return pltpu.make_async_remote_copy(
            src_ref=rfull.at[rows, :], dst_ref=rfull.at[rows, :],
            send_sem=dg_send.at[k - 1], recv_sem=dg_recv.at[k - 1],
            device_id=(lax.rem(d + k, n), e), device_id_type=MESH,
        )

    def gather_e(k, source):
        rows = pl.ds(pl.multiple_of(source * piece_e, piece_e), piece_e)
        return pltpu.make_async_remote_copy(
            src_ref=rfull.at[rows, :], dst_ref=rfull.at[rows, :],
            send_sem=eg_send.at[k - 1], recv_sem=eg_recv.at[k - 1],
            device_id=(d, lax.rem(e + k, flight)), device_id_type=MESH,
        )

    cap = home_dx.shape[1]

    def block(ref, index):
        return ref.at[pl.ds(pl.multiple_of(index * cap, cap), cap), :]

    def give_score(k, source):
        to = lax.rem(e + k, flight)
        return pltpu.make_async_remote_copy(
            src_ref=block(score_ref, to), dst_ref=home_score.at[source],
            send_sem=sc_send.at[k - 1], recv_sem=sc_recv.at[k - 1],
            device_id=(d, to), device_id_type=MESH,
        )

    def give_dx(k, source):
        to = lax.rem(e + k, flight)
        return pltpu.make_async_remote_copy(
            src_ref=block(back, to), dst_ref=home_dx.at[source],
            send_sem=dx_send.at[k - 1], recv_sem=dx_recv.at[k - 1],
            device_id=(d, to), device_id_type=MESH,
        )

    def from_peer(k):
        return lax.rem(e + flight - k, flight)

    def one_hot(k):
        spots = lax.broadcasted_iota(jnp.int32, (ids_ref.shape[0], flight * cap), 1)
        return spots == ids_ref[:, top + k:top + k + 1]

    top = ids_ref.shape[1] // 2
    for part in range(3):
        for way in range(2):
            slot(way, part, 0)[...] = own(way, part, owner_at(way, 0)).astype(BF16)
            hop(way, part, 0).start()
    for k in range(1, flight):
        give_score(k, e).start()
    home_score[e] = score_ref[pl.ds(pl.multiple_of(e * cap, cap), cap), :]

    load_w.wait()
    width = back.shape[1]
    tile = min(width, 512)
    for col in range(0, width, tile):
        back[:, col:col + tile] = lax.dot_general(
            pg_ref[...], wg_ref[col:col + tile, :], (((1,), (1,)), ((), ())),
            preferred_element_type=F32,
        ).astype(BF16)
    home_dx[e] = back[pl.ds(pl.multiple_of(e * cap, cap), cap), :]
    for k in range(1, flight):
        give_dx(k, e).start()

    def middle(step, carry):
        for part in range(3):
            for way in range(2):
                hop(way, part, step - 1).wait_recv()
                here = slot(way, part, step)
                here[...] = (
                    here[...].astype(F32) + own(way, part, owner_at(way, step))
                ).astype(BF16)
                hop(way, part, step).start()

        @pl.when(step == 1)
        def _():
            for k in range(1, flight):
                give_score(k, from_peer(k)).wait_recv()
            arrived = home_score[...].reshape(flight * cap, home_score.shape[2])
            logits = logit_ref[...]
            lanes = lax.broadcasted_iota(jnp.int32, logits.shape, 1)
            scores = [
                jnp.dot(
                    one_hot(k).astype(F32), arrived,
                    precision=lax.Precision.HIGHEST, preferred_element_type=F32,
                )
                for k in range(top)
            ]
            probs = [small_ref[:, k:k + 1] for k in range(top)]
            mean = sum(p * q for p, q in zip(probs, scores))
            z_weight = small_ref[:, top:top + 1]
            log_total = small_ref[:, top + 1:top + 2]
            grad = 2.0 * z_weight * log_total * jnp.exp(logits - log_total)
            for k in range(top):
                grad = grad + jnp.where(
                    ids_ref[:, k:k + 1] == lanes, probs[k] * (scores[k] - mean), 0.0
                )
            lg_ref[...] = grad.astype(BF16)
            rp_ref[...] = jnp.dot(tokt_ref[...], lg_ref[...], preferred_element_type=F32)
            for k in range(1, flight):
                share_e(k).start()

        @pl.when(step == 2)
        def _():
            total = rp_ref[pl.ds(pl.multiple_of(e * piece_e, piece_e), piece_e), :]
            for k in range(1, flight):
                share_e(k).wait_recv()
                total = total + rx_e[k - 1]
            rsum[...] = total
            for k in range(1, n):
                share_d(k).start()

        @pl.when(step == 3)
        def _():
            total = rsum[pl.ds(pl.multiple_of(d * piece_d, piece_d), piece_d), :]
            for k in range(1, n):
                share_d(k).wait_recv()
                total = total + rx_d[k - 1]
            rfull[pl.ds(pl.multiple_of(e * piece_e + d * piece_d, piece_d), piece_d), :] = total
            for k in range(1, n):
                gather_d(k, d).start()

        @pl.when(step == 4)
        def _():
            for k in range(1, n):
                gather_d(k, lax.rem(d + n - k, n)).wait_recv()
            for k in range(1, flight):
                gather_e(k, e).start()

        @pl.when(step == 5)
        def _():
            for k in range(1, flight):
                give_dx(k, from_peer(k)).wait_recv()
            picks = sum(one_hot(k).astype(F32) for k in range(top)).astype(BF16)
            rows = home_dx[...].reshape(flight * cap, width)
            for col in range(0, width, tile):
                total = jnp.dot(picks, rows[:, col:col + tile], preferred_element_type=F32)
                total = total + lax.dot_general(
                    lg_ref[...], rw_ref[col:col + tile, :], (((1,), (1,)), ((), ())),
                    preferred_element_type=F32,
                )
                tg_ref[:, col:col + tile] = total.astype(BF16)

        return carry

    lax.fori_loop(1, n - 1, middle, 0)

    for k in range(1, flight):
        gather_e(k, from_peer(k)).wait_recv()
    rout_ref[...] = rfull[...]
    for part in range(3):
        for way in range(2):
            hop(way, part, n - 2).wait_recv()
            total = slot(way, part, n - 1)[...].astype(F32) + own(way, part, d)
            if part < 2:
                gu_ref[
                    0, part * half_rows:(part + 1) * half_rows, way * gu_cols:(way + 1) * gu_cols
                ] = total.astype(BF16)
            else:
                dn_ref[0, :, way * dn_cols:(way + 1) * dn_cols] = total.astype(BF16)

    def drain(step, carry):
        for part in range(3):
            for way in range(2):
                hop(way, part, step).wait_send()
        return carry

    lax.fori_loop(0, n - 1, drain, 0)
    for k in range(1, n):
        share_d(k).wait_send()
        gather_d(k, d).wait_send()
    for k in range(1, flight):
        share_e(k).wait_send()
        gather_e(k, e).wait_send()
        give_score(k, e).wait_send()
        give_dx(k, e).wait_send()


def reduce_grads(
    copies, flight, xt, pre_grad, ht, dyk, score, w_gateup, tokt, router_weight, logits, small, ids
):
    width, rows = xt.shape
    gate_up = pre_grad.shape[1]
    hidden = ht.shape[0]
    tok_count, routed = logits.shape
    cap = rows // flight
    n = copies
    gu_rows, dn_rows = width // n, hidden // n
    piece_e = width // flight
    piece_d = piece_e // n
    dma = pltpu.SemaphoreType.DMA
    vmem = pl.BlockSpec(memory_space=pltpu.VMEM)
    return pl.pallas_call(
        functools.partial(grads_kernel, n, flight, ring_order(n)),
        out_shape=(
            jax.ShapeDtypeStruct((1, gu_rows, gate_up), BF16),
            jax.ShapeDtypeStruct((1, dn_rows, width), BF16),
            jax.ShapeDtypeStruct((width, routed), F32),
            jax.ShapeDtypeStruct((tok_count, width), BF16),
        ),
        in_specs=[vmem] * 5 + [pl.BlockSpec(memory_space=pl.ANY)] + [vmem] * 5,
        out_specs=(vmem,) * 4,
        scratch_shapes=[
            pltpu.VMEM((2, 2, n, gu_rows // 2, gate_up // 2), BF16),
            pltpu.VMEM((2, n, dn_rows, width // 2), BF16),
            pltpu.VMEM((flight - 1, piece_e, routed), F32),
            pltpu.VMEM((piece_e, routed), F32),
            pltpu.VMEM((n - 1, piece_d, routed), F32),
            pltpu.VMEM((width, routed), F32),
            pltpu.VMEM((width, routed), F32),
            pltpu.VMEM(w_gateup.shape, BF16),
            pltpu.VMEM((rows, width), BF16),
            pltpu.VMEM((flight, cap, width), BF16),
            pltpu.VMEM((flight, cap, routed), F32),
            pltpu.VMEM((tok_count, routed), BF16),
            dma((2, 3, n - 1)), dma((2, 3, n - 1)),
            dma((flight - 1,)), dma((flight - 1,)),
            dma((n - 1,)), dma((n - 1,)),
            dma((n - 1,)), dma((n - 1,)),
            dma((flight - 1,)), dma((flight - 1,)),
            dma, dma((flight - 1,)), dma((flight - 1,)),
            dma((flight - 1,)), dma((flight - 1,)),
        ],
        compiler_params=pltpu.CompilerParams(
            collective_id=0, has_side_effects=True, vmem_limit_bytes=58 * 2**20
        ),
        cost_estimate=pl.CostEstimate(
            flops=2 * rows * width * (gate_up + hidden),
            bytes_accessed=2 * (width * gate_up + hidden * width) // n,
            transcendentals=0,
        ),
        name="grads",
    )(xt, pre_grad, ht, dyk, score, w_gateup, tokt, router_weight, logits, small, ids)

def expert_rows(rows_in, rows_raw, row_prob, w_gateup, w_down):
    hidden_units = w_down.shape[0]
    pre_act = jnp.dot(rows_in, w_gateup, preferred_element_type=F32)
    gate_pre = pre_act[:, :hidden_units]
    up_pre = pre_act[:, hidden_units:]
    activated = jax.nn.silu(gate_pre)
    hidden = (activated * up_pre).astype(BF16)
    raw_grad = lax.dot_general(
        rows_raw, w_down, (((1,), (1,)), ((), ())), preferred_element_type=F32
    )
    score = jnp.sum(raw_grad * hidden.astype(F32), axis=1)
    hidden_grad = row_prob[:, None] * raw_grad
    sigmoid_gate = jax.nn.sigmoid(gate_pre)
    gate_grad = hidden_grad * up_pre * sigmoid_gate * (1.0 + gate_pre * (1.0 - sigmoid_gate))
    up_grad = hidden_grad * activated
    pre_grad = jnp.concatenate([gate_grad, up_grad], axis=1).astype(BF16)
    return (hidden, pre_grad, score)


def split_pair(values):
    upper = values.astype(jnp.bfloat16)
    lower = (values - upper.astype(jnp.float32)).astype(jnp.bfloat16)
    return jnp.stack([upper, lower], axis=-1)


def join_pair(pair):
    return pair[..., 0].astype(jnp.float32) + pair[..., 1].astype(jnp.float32)


def per_device(tokens, out_grad, z_weight, router_weight, expert_ids, gate_up_weight, down_weight):
    tok_count, width = tokens.shape
    top_count = expert_ids.shape[1]
    routed = router_weight.shape[1]
    flight = lax.axis_size("expert")
    capacity = tok_count // 2
    w_gateup = gate_up_weight[0]
    w_down = down_weight[0]
    hidden_units = w_down.shape[0]
    logits = jnp.dot(tokens, router_weight, preferred_element_type=jnp.float32)
    choose = expert_ids[:, :, None] == jnp.arange(routed, dtype=jnp.int32)[None, None, :]
    selected = jnp.sum(jnp.where(choose, logits[:, None, :], 0.0), axis=2)
    sel_exp = jnp.exp(selected)
    probs = sel_exp / jnp.sum(sel_exp, axis=1, keepdims=True)
    log_total = jnp.log(jnp.sum(jnp.exp(logits), axis=1))
    flat_ids = expert_ids.reshape(-1)
    slot_count = tok_count * top_count
    member = (flat_ids[:, None] == jnp.arange(flight, dtype=jnp.int32)[None, :]).astype(jnp.int32)
    ranks = jnp.sum((jnp.cumsum(member, axis=0) - 1) * member, axis=1)
    in_flight = flat_ids < flight
    position = jnp.where(in_flight, flat_ids * capacity + ranks, flight * capacity)
    source_slot = (
        jnp.zeros((flight * capacity,), jnp.int32)
        .at[position]
        .set(jnp.arange(slot_count, dtype=jnp.int32), mode="drop")
    )
    filled = jnp.zeros((flight * capacity,), jnp.bool_).at[position].set(True, mode="drop")
    source_tok = source_slot // top_count
    send_in = jnp.where(filled[:, None], tokens[source_tok], 0)
    slot_prob = jnp.where(filled, probs.reshape(-1)[source_slot], 0.0)
    counts = jnp.sum(member, axis=0)
    count_msg = jnp.stack([counts // 128, counts % 128], axis=1).astype(jnp.bfloat16)
    send_raw = jnp.where(filled[:, None], out_grad[source_tok], 0)
    prob_pair = split_pair(slot_prob)
    recv_in, recv_raw, recv_prob, recv_counts = (
        lax.all_to_all(
            send_in.reshape(flight, capacity, width),
            "expert",
            split_axis=0,
            concat_axis=0,
            tiled=True,
        ),
        lax.all_to_all(
            send_raw.reshape(flight, capacity, width),
            "expert",
            split_axis=0,
            concat_axis=0,
            tiled=True,
        ),
        lax.all_to_all(
            prob_pair.reshape(flight, capacity, 2),
            "expert",
            split_axis=0,
            concat_axis=0,
            tiled=True,
        ),
        lax.all_to_all(count_msg, "expert", split_axis=0, concat_axis=0, tiled=True),
    )
    sources = recv_in.shape[0]
    total_rows = sources * capacity
    flat_in = recv_in.reshape(total_rows, width)
    flat_raw = recv_raw.reshape(total_rows, width)
    row_prob = join_pair(recv_prob.reshape(total_rows, 2))
    flat_grad = (row_prob[:, None] * flat_raw.astype(jnp.float32)).astype(jnp.bfloat16)
    hidden, pre_grad, score = expert_rows(flat_in, flat_raw, row_prob, w_gateup, w_down)
    spot = jnp.where(in_flight, position, -1).reshape(tok_count, top_count)
    small = jnp.concatenate([probs, z_weight[:, None], log_total[:, None]], axis=1)
    gate_up_grad, down_grad, router_grad, token_grad = reduce_grads(
        lax.axis_size("dp"),
        flight,
        flat_in.T,
        pre_grad,
        hidden.T,
        flat_grad,
        jnp.broadcast_to(score[:, None], (total_rows, routed)),
        w_gateup,
        tokens.T,
        router_weight,
        logits,
        small,
        jnp.concatenate([expert_ids, spot], axis=1),
    )
    return (token_grad, router_grad, gate_up_grad, down_grad)


def solution(mesh):
    return jax.shard_map(
        per_device,
        mesh=mesh,
        in_specs=(
            P(("dp", "expert"), None),
            P(("dp", "expert"), None),
            P(("dp", "expert")),
            P(),
            P(("dp", "expert"), None),
            P("expert", None, None),
            P("expert", None, None),
        ),
        out_specs=(
            P(("dp", "expert"), None),
            P(),
            P("expert", "dp", None),
            P("expert", "dp", None),
        ),
        check_vma=False,
    )
```

```python
import functools

import jax
import jax.numpy as jnp
from jax import lax
from jax.experimental import pallas as pl
from jax.experimental.pallas import tpu as pltpu
from jax.sharding import PartitionSpec as P

F32 = jnp.float32
BF16 = jnp.bfloat16
MESH = pl.DeviceIdType.MESH


def ring_order(count):
    inner = max(k for k in range(1, count + 1) if count % k == 0 and k * k <= count)
    outer = count // inner
    if inner == 1 or outer % 2:
        return list(range(count))
    order = []
    for row in range(outer):
        cols = list(range(1, inner))
        order += [row * inner + col for col in (cols if row % 2 == 0 else cols[::-1])]
    return order + [row * inner for row in range(outer)][::-1]


def lookup(table, key):
    value = jnp.int32(0)
    for slot, entry in enumerate(table):
        value = value + jnp.where(key == slot, jnp.int32(entry), jnp.int32(0))
    return value


def grads_kernel(
    copies, flight, order,
    xt_ref, pg_ref, ht_ref, dy_ref, score_ref, wg_hbm, tokt_ref, rw_ref, logit_ref, small_ref, ids_ref, spot_ref, zw_ref,
    gu_ref, dn_ref, rout_ref, tg_ref,
    gu_buf, dn_buf, rx_e, rsum, rx_d, rfull, rp_ref, wg_ref, back, home_dx, home_score, lg_ref,
    send_sem, recv_sem, es_send, es_recv, ds_send, ds_recv, dg_send, dg_recv, eg_send, eg_recv,
    wg_sem, dx_send, dx_recv, sc_send, sc_recv,
):
    d = lax.axis_index("dp")
    e = lax.axis_index("expert")
    n = copies
    place = [order.index(i) for i in range(n)]
    pos = lookup(place, d)
    right = lookup(order, lax.rem(pos + 1, n))
    left = lookup(order, lax.rem(pos + n - 1, n))
    towards = (right, left)

    load_w = pltpu.make_async_copy(wg_hbm, wg_ref, wg_sem)
    load_w.start()
    barrier = pltpu.get_barrier_semaphore()
    for k in range(1, n):
        pl.semaphore_signal(barrier, inc=1, device_id=(lax.rem(d + k, n), e), device_id_type=MESH)
    for k in range(1, flight):
        pl.semaphore_signal(barrier, inc=1, device_id=(d, lax.rem(e + k, flight)), device_id_type=MESH)
    pl.semaphore_wait(barrier, n + flight - 2)

    gu_rows = gu_ref.shape[1]
    half_rows = gu_rows // 2
    dn_rows = dn_ref.shape[1]
    gu_cols = gu_ref.shape[2] // 2
    dn_cols = dn_ref.shape[2] // 2
    piece_e = rsum.shape[0]
    piece_d = rx_d.shape[1]

    def owner_at(way, step):
        if way == 0:
            return lookup(order, lax.rem(pos + 2 * n - 1 - step, n))
        return lookup(order, lax.rem(pos + 1 + step, n))

    def own(way, part, owner):
        if part < 2:
            start = pl.multiple_of(owner * gu_rows + part * half_rows, half_rows)
            return jnp.dot(
                xt_ref[pl.ds(start, half_rows), :],
                pg_ref[:, way * gu_cols:(way + 1) * gu_cols],
                preferred_element_type=F32,
            )
        start = pl.multiple_of(owner * dn_rows, dn_rows)
        return jnp.dot(
            ht_ref[pl.ds(start, dn_rows), :],
            dy_ref[:, way * dn_cols:(way + 1) * dn_cols],
            preferred_element_type=F32,
        )

    def slot(way, part, step):
        return gu_buf.at[way, part, step] if part < 2 else dn_buf.at[way, step]

    def hop(way, part, step):
        return pltpu.make_async_remote_copy(
            src_ref=slot(way, part, step),
            dst_ref=slot(way, part, step + 1),
            send_sem=send_sem.at[way, part, step],
            recv_sem=recv_sem.at[way, part, step],
            device_id=(towards[way], e),
            device_id_type=MESH,
        )

    def share_e(k):
        to = lax.rem(e + k, flight)
        return pltpu.make_async_remote_copy(
            src_ref=rp_ref.at[pl.ds(pl.multiple_of(to * piece_e, piece_e), piece_e), :],
            dst_ref=rx_e.at[k - 1],
            send_sem=es_send.at[k - 1], recv_sem=es_recv.at[k - 1],
            device_id=(d, to), device_id_type=MESH,
        )

    def share_d(k):
        to = lax.rem(d + k, n)
        return pltpu.make_async_remote_copy(
            src_ref=rsum.at[pl.ds(pl.multiple_of(to * piece_d, piece_d), piece_d), :],
            dst_ref=rx_d.at[k - 1],
            send_sem=ds_send.at[k - 1], recv_sem=ds_recv.at[k - 1],
            device_id=(to, e), device_id_type=MESH,
        )

    def gather_d(k, source):
        rows = pl.ds(pl.multiple_of(e * piece_e + source * piece_d, piece_d), piece_d)
        return pltpu.make_async_remote_copy(
            src_ref=rfull.at[rows, :], dst_ref=rfull.at[rows, :],
            send_sem=dg_send.at[k - 1], recv_sem=dg_recv.at[k - 1],
            device_id=(lax.rem(d + k, n), e), device_id_type=MESH,
        )

    def gather_e(k, source):
        rows = pl.ds(pl.multiple_of(source * piece_e, piece_e), piece_e)
        return pltpu.make_async_remote_copy(
            src_ref=rfull.at[rows, :], dst_ref=rfull.at[rows, :],
            send_sem=eg_send.at[k - 1], recv_sem=eg_recv.at[k - 1],
            device_id=(d, lax.rem(e + k, flight)), device_id_type=MESH,
        )

    cap = home_dx.shape[1]

    def block(ref, index):
        return ref.at[pl.ds(pl.multiple_of(index * cap, cap), cap), :]

    def give_score(k, source):
        to = lax.rem(e + k, flight)
        return pltpu.make_async_remote_copy(
            src_ref=block(score_ref, to), dst_ref=home_score.at[source],
            send_sem=sc_send.at[k - 1], recv_sem=sc_recv.at[k - 1],
            device_id=(d, to), device_id_type=MESH,
        )

    def give_dx(k, source):
        to = lax.rem(e + k, flight)
        return pltpu.make_async_remote_copy(
            src_ref=block(back, to), dst_ref=home_dx.at[source],
            send_sem=dx_send.at[k - 1], recv_sem=dx_recv.at[k - 1],
            device_id=(d, to), device_id_type=MESH,
        )

    def from_peer(k):
        return lax.rem(e + flight - k, flight)

    def one_hot(k):
        spots = lax.broadcasted_iota(jnp.int32, (ids_ref.shape[0], flight * cap), 1)
        return spots == spot_ref[:, k:k + 1]

    top = ids_ref.shape[1]
    for part in range(3):
        for way in range(2):
            slot(way, part, 0)[...] = own(way, part, owner_at(way, 0)).astype(BF16)
            hop(way, part, 0).start()
    for k in range(1, flight):
        give_score(k, e).start()
    home_score[e] = score_ref[pl.ds(pl.multiple_of(e * cap, cap), cap), :]

    load_w.wait()
    width = back.shape[1]
    tile = min(width, 512)
    for col in range(0, width, tile):
        back[:, col:col + tile] = lax.dot_general(
            pg_ref[...], wg_ref[col:col + tile, :], (((1,), (1,)), ((), ())),
            preferred_element_type=F32,
        ).astype(BF16)
    home_dx[e] = back[pl.ds(pl.multiple_of(e * cap, cap), cap), :]
    for k in range(1, flight):
        give_dx(k, e).start()

    def middle(step, carry):
        for part in range(3):
            for way in range(2):
                hop(way, part, step - 1).wait_recv()
                here = slot(way, part, step)
                here[...] = (
                    here[...].astype(F32) + own(way, part, owner_at(way, step))
                ).astype(BF16)
                hop(way, part, step).start()

        @pl.when(step == 1)
        def _():
            for k in range(1, flight):
                give_score(k, from_peer(k)).wait_recv()
            arrived = home_score[...].reshape(flight * cap, home_score.shape[2])
            logits = logit_ref[...]
            lanes = lax.broadcasted_iota(jnp.int32, logits.shape, 1)
            scores = [
                jnp.dot(
                    one_hot(k).astype(F32), arrived,
                    precision=lax.Precision.HIGHEST, preferred_element_type=F32,
                )
                for k in range(top)
            ]
            probs = [small_ref[:, k:k + 1] for k in range(top)]
            mean = sum(p * q for p, q in zip(probs, scores))
            z_weight = zw_ref[...]
            log_total = small_ref[:, top:top + 1]
            grad = 2.0 * z_weight * log_total * jnp.exp(logits - log_total)
            for k in range(top):
                grad = grad + jnp.where(
                    ids_ref[:, k:k + 1] == lanes, probs[k] * (scores[k] - mean), 0.0
                )
            lg_ref[...] = grad.astype(BF16)
            rp_ref[...] = jnp.dot(tokt_ref[...], lg_ref[...], preferred_element_type=F32)
            for k in range(1, flight):
                share_e(k).start()

        @pl.when(step == 2)
        def _():
            total = rp_ref[pl.ds(pl.multiple_of(e * piece_e, piece_e), piece_e), :]
            for k in range(1, flight):
                share_e(k).wait_recv()
                total = total + rx_e[k - 1]
            rsum[...] = total
            for k in range(1, n):
                share_d(k).start()

        @pl.when(step == 3)
        def _():
            total = rsum[pl.ds(pl.multiple_of(d * piece_d, piece_d), piece_d), :]
            for k in range(1, n):
                share_d(k).wait_recv()
                total = total + rx_d[k - 1]
            rfull[pl.ds(pl.multiple_of(e * piece_e + d * piece_d, piece_d), piece_d), :] = total
            for k in range(1, n):
                gather_d(k, d).start()

        @pl.when(step == 4)
        def _():
            for k in range(1, n):
                gather_d(k, lax.rem(d + n - k, n)).wait_recv()
            for k in range(1, flight):
                gather_e(k, e).start()

        @pl.when(step == 5)
        def _():
            for k in range(1, flight):
                give_dx(k, from_peer(k)).wait_recv()
            picks = sum(one_hot(k).astype(F32) for k in range(top)).astype(BF16)
            rows = home_dx[...].reshape(flight * cap, width)
            for col in range(0, width, tile):
                total = jnp.dot(picks, rows[:, col:col + tile], preferred_element_type=F32)
                total = total + lax.dot_general(
                    lg_ref[...], rw_ref[col:col + tile, :], (((1,), (1,)), ((), ())),
                    preferred_element_type=F32,
                )
                tg_ref[:, col:col + tile] = total.astype(BF16)

        return carry

    lax.fori_loop(1, n - 1, middle, 0)

    for k in range(1, flight):
        gather_e(k, from_peer(k)).wait_recv()
    rout_ref[...] = rfull[...]
    for part in range(3):
        for way in range(2):
            hop(way, part, n - 2).wait_recv()
            total = slot(way, part, n - 1)[...].astype(F32) + own(way, part, d)
            if part < 2:
                gu_ref[
                    0, part * half_rows:(part + 1) * half_rows, way * gu_cols:(way + 1) * gu_cols
                ] = total.astype(BF16)
            else:
                dn_ref[0, :, way * dn_cols:(way + 1) * dn_cols] = total.astype(BF16)

    def drain(step, carry):
        for part in range(3):
            for way in range(2):
                hop(way, part, step).wait_send()
        return carry

    lax.fori_loop(0, n - 1, drain, 0)
    for k in range(1, n):
        share_d(k).wait_send()
        gather_d(k, d).wait_send()
    for k in range(1, flight):
        share_e(k).wait_send()
        gather_e(k, e).wait_send()
        give_score(k, e).wait_send()
        give_dx(k, e).wait_send()


def reduce_grads(
    copies, flight, xt, pre_grad, ht, dyk, score, w_gateup, tokt, router_weight, logits, small, ids,
    spot, zw,
):
    width, rows = xt.shape
    gate_up = pre_grad.shape[1]
    hidden = ht.shape[0]
    tok_count, routed = logits.shape
    cap = rows // flight
    n = copies
    gu_rows, dn_rows = width // n, hidden // n
    piece_e = width // flight
    piece_d = piece_e // n
    dma = pltpu.SemaphoreType.DMA
    vmem = pl.BlockSpec(memory_space=pltpu.VMEM)
    return pl.pallas_call(
        functools.partial(grads_kernel, n, flight, ring_order(n)),
        out_shape=(
            jax.ShapeDtypeStruct((1, gu_rows, gate_up), BF16),
            jax.ShapeDtypeStruct((1, dn_rows, width), BF16),
            jax.ShapeDtypeStruct((width, routed), F32),
            jax.ShapeDtypeStruct((tok_count, width), BF16),
        ),
        in_specs=[vmem] * 5 + [pl.BlockSpec(memory_space=pl.ANY)] + [vmem] * 7,
        out_specs=(vmem,) * 4,
        scratch_shapes=[
            pltpu.VMEM((2, 2, n, gu_rows // 2, gate_up // 2), BF16),
            pltpu.VMEM((2, n, dn_rows, width // 2), BF16),
            pltpu.VMEM((flight - 1, piece_e, routed), F32),
            pltpu.VMEM((piece_e, routed), F32),
            pltpu.VMEM((n - 1, piece_d, routed), F32),
            pltpu.VMEM((width, routed), F32),
            pltpu.VMEM((width, routed), F32),
            pltpu.VMEM(w_gateup.shape, BF16),
            pltpu.VMEM((rows, width), BF16),
            pltpu.VMEM((flight, cap, width), BF16),
            pltpu.VMEM((flight, cap, routed), F32),
            pltpu.VMEM((tok_count, routed), BF16),
            dma((2, 3, n - 1)), dma((2, 3, n - 1)),
            dma((flight - 1,)), dma((flight - 1,)),
            dma((n - 1,)), dma((n - 1,)),
            dma((n - 1,)), dma((n - 1,)),
            dma((flight - 1,)), dma((flight - 1,)),
            dma, dma((flight - 1,)), dma((flight - 1,)),
            dma((flight - 1,)), dma((flight - 1,)),
        ],
        compiler_params=pltpu.CompilerParams(
            collective_id=0, has_side_effects=True, vmem_limit_bytes=58 * 2**20
        ),
        cost_estimate=pl.CostEstimate(
            flops=2 * rows * width * (gate_up + hidden),
            bytes_accessed=2 * (width * gate_up + hidden * width) // n,
            transcendentals=0,
        ),
        name="grads",
    )(xt, pre_grad, ht, dyk, score, w_gateup, tokt, router_weight, logits, small, ids, spot, zw)

def rows_kernel(
    flight, cap,
    tok_ref, og_ref, rw_ref, ids_ref, wg_hbm, wd_hbm,
    xt_ref, ht_ref, pg_ref, dy_ref, score_ref, logit_ref, small_ref, spot_ref,
    wg_ref, wd_ref, out_x, out_o, out_p, in_x, in_o, in_p, pre, hid,
    wg_sem, wd_sem, x_send, x_recv, o_send, o_recv, p_send, p_recv,
):
    d = lax.axis_index("dp")
    e = lax.axis_index("expert")
    load_g = pltpu.make_async_copy(wg_hbm, wg_ref, wg_sem)
    load_d = pltpu.make_async_copy(wd_hbm, wd_ref, wd_sem)
    load_g.start()
    load_d.start()
    barrier = pltpu.get_barrier_semaphore()
    for k in range(1, flight):
        pl.semaphore_signal(barrier, inc=1, device_id=(d, lax.rem(e + k, flight)), device_id_type=MESH)

    tok_count, top = ids_ref.shape
    routed = rw_ref.shape[1]
    hidden_units, width = wd_ref.shape
    tile = min(hidden_units, 512)
    pairs = flight // 2
    lanes = lax.broadcasted_iota(jnp.int32, (tok_count, routed), 1)
    choose = [ids_ref[:, k:k + 1] == lanes for k in range(top)]
    member = sum(c.astype(F32) for c in choose)
    earlier = lax.broadcasted_iota(jnp.int32, (tok_count, tok_count), 0) > (
        lax.broadcasted_iota(jnp.int32, (tok_count, tok_count), 1)
    )
    rank = jnp.dot(earlier.astype(F32).astype(BF16), member.astype(BF16), preferred_element_type=F32)
    rank = jnp.where(member > 0.0, rank, -1.0)
    by_expert = rank.T.astype(jnp.int32)
    ranks = lax.broadcasted_iota(jnp.int32, (cap, tok_count), 0)
    picks = [by_expert[f:f + 1, :] == ranks for f in range(flight)]

    pl.semaphore_wait(barrier, flight - 1)

    def rows_of(index):
        return pl.ds(pl.multiple_of(index * cap, cap), cap)

    def peers():
        found = []
        for i in range(1, pairs):
            pair = lax.rem(lax.div(e, 2) + i, pairs)
            found += [pair * 2 + lax.rem(e, 2), pair * 2 + 1 - lax.rem(e, 2)]
        return found + [lax.div(e, 2) * 2 + 1 - lax.rem(e, 2)]

    def give(out, into, sends, recvs, source, target):
        return pltpu.make_async_remote_copy(
            src_ref=out.at[rows_of(target), :], dst_ref=into.at[rows_of(source), :],
            send_sem=sends.at[target], recv_sem=recvs.at[source],
            device_id=(d, target), device_id_type=MESH,
        )

    give_x = functools.partial(give, out_x, in_x, x_send, x_recv)
    give_o = functools.partial(give, out_o, in_o, o_send, o_recv)
    give_p = functools.partial(give, out_p, in_p, p_send, p_recv)

    for f in range(flight):
        out_x[f * cap:(f + 1) * cap, :] = jnp.dot(
            picks[f].astype(F32).astype(BF16), tok_ref[...], preferred_element_type=F32
        ).astype(BF16)
    for to in peers():
        give_x(e, to).start()
    for f in range(flight):
        out_o[f * cap:(f + 1) * cap, :] = jnp.dot(
            picks[f].astype(F32).astype(BF16), og_ref[...], preferred_element_type=F32
        ).astype(BF16)
    for to in peers():
        give_o(e, to).start()

    logits = jnp.dot(tok_ref[...], rw_ref[...], preferred_element_type=F32)
    logit_ref[...] = logits
    chosen = [
        jnp.exp(jnp.sum(jnp.where(c, logits, 0.0), axis=1, keepdims=True)) for c in choose
    ]
    norm = sum(chosen)
    probs = [c / norm for c in chosen]
    log_total = jnp.log(jnp.sum(jnp.exp(logits), axis=1, keepdims=True))
    small = jnp.where(lanes == top, log_total, 0.0)
    spot = jnp.full(lanes.shape, -1, jnp.int32)
    weight = jnp.zeros(lanes.shape, F32)
    place = jnp.where((rank >= 0.0) & (lanes < flight), rank + (lanes * cap).astype(F32) + 1.0, 0.0)
    for k in range(top):
        small = jnp.where(lanes == k, probs[k], small)
        at = jnp.sum(jnp.where(choose[k], place, 0.0), axis=1, keepdims=True) - 1.0
        spot = jnp.where(lanes == k, at.astype(jnp.int32), spot)
        weight = weight + jnp.where(choose[k], probs[k], 0.0)
    small_ref[...] = small
    spot_ref[...] = spot
    weight = weight.T
    for f in range(flight):
        row = jnp.sum(jnp.where(picks[f], weight[f:f + 1, :], 0.0), axis=1, keepdims=True)
        out_p[f * cap:(f + 1) * cap, :] = jnp.broadcast_to(row, (cap, routed))
    for to in peers():
        give_p(e, to).start()
    in_x[rows_of(e), :] = out_x[rows_of(e), :]
    in_o[rows_of(e), :] = out_o[rows_of(e), :]
    in_p[rows_of(e), :] = out_p[rows_of(e), :]

    def arrived(gives, pair):
        for core in range(2):
            source = pair * 2 + core

            @pl.when(source != e)
            def _():
                for g in gives:
                    g(source, e).wait_recv()

    def pair_rows(pair):
        return pl.ds(pl.multiple_of(pair * (2 * cap), 2 * cap), 2 * cap)

    load_g.wait()

    def forward(i, carry):
        pair = lax.rem(lax.div(e, 2) + i, pairs)
        arrived([give_x], pair)
        rows = pair_rows(pair)
        for col in range(0, 2 * hidden_units, tile):
            pre[rows, col:col + tile] = jnp.dot(
                in_x[rows, :], wg_ref[:, col:col + tile], preferred_element_type=F32
            )
        return carry

    lax.fori_loop(0, pairs, forward, 0)
    load_d.wait()

    def backward(i, carry):
        pair = lax.rem(lax.div(e, 2) + i, pairs)
        arrived([give_o, give_p], pair)
        rows = pair_rows(pair)
        prob = in_p[rows, 0:1]
        score = jnp.zeros((2 * cap, 1), F32)
        for col in range(0, hidden_units, tile):
            raw = lax.dot_general(
                in_o[rows, :], wd_ref[col:col + tile, :], (((1,), (1,)), ((), ())),
                preferred_element_type=F32,
            )
            gate = pre[rows, col:col + tile]
            up = pre[rows, hidden_units + col:hidden_units + col + tile]
            sig = jax.nn.sigmoid(gate)
            active = gate * sig
            hidden = (active * up).astype(BF16)
            hid[rows, col:col + tile] = hidden
            score = score + jnp.sum(raw * hidden.astype(F32), axis=1, keepdims=True)
            grad = prob * raw
            pg_ref[rows, col:col + tile] = (
                grad * up * sig * (1.0 + gate * (1.0 - sig))
            ).astype(BF16)
            pg_ref[rows, hidden_units + col:hidden_units + col + tile] = (grad * active).astype(BF16)
        score_ref[rows, :] = jnp.broadcast_to(score, (2 * cap, routed))
        dy_ref[rows, :] = (prob * in_o[rows, :].astype(F32)).astype(BF16)
        return carry

    xt_ref[...] = in_x[...].T
    lax.fori_loop(0, pairs, backward, 0)
    ht_ref[...] = hid[...].T
    for to in peers():
        give_x(e, to).wait_send()
        give_o(e, to).wait_send()
        give_p(e, to).wait_send()


def expert_rows(flight, tokens, out_grad, router_weight, ids, w_gateup, w_down):
    tok_count, width = tokens.shape
    routed = router_weight.shape[1]
    hidden = w_down.shape[0]
    cap = tok_count // 2
    rows = flight * cap
    dma = pltpu.SemaphoreType.DMA
    vmem = pl.BlockSpec(memory_space=pltpu.VMEM)
    hbm = pl.BlockSpec(memory_space=pl.ANY)
    shape = jax.ShapeDtypeStruct
    return pl.pallas_call(
        functools.partial(rows_kernel, flight, cap),
        out_shape=(
            shape((width, rows), BF16),
            shape((hidden, rows), BF16),
            shape((rows, 2 * hidden), BF16),
            shape((rows, width), BF16),
            shape((rows, routed), F32),
            shape((tok_count, routed), F32),
            shape((tok_count, routed), F32),
            shape((tok_count, routed), jnp.int32),
        ),
        in_specs=[vmem] * 4 + [hbm] * 2,
        out_specs=(vmem,) * 8,
        scratch_shapes=[
            pltpu.VMEM(w_gateup.shape, BF16),
            pltpu.VMEM(w_down.shape, BF16),
            pltpu.VMEM((rows, width), BF16),
            pltpu.VMEM((rows, width), BF16),
            pltpu.VMEM((rows, routed), F32),
            pltpu.VMEM((rows, width), BF16),
            pltpu.VMEM((rows, width), BF16),
            pltpu.VMEM((rows, routed), F32),
            pltpu.VMEM((rows, 2 * hidden), F32),
            pltpu.VMEM((rows, hidden), BF16),
            dma, dma,
        ] + [dma((flight,))] * 6,
        compiler_params=pltpu.CompilerParams(
            collective_id=1, has_side_effects=True, vmem_limit_bytes=58 * 2**20
        ),
        cost_estimate=pl.CostEstimate(
            flops=6 * rows * width * hidden,
            bytes_accessed=6 * width * hidden,
            transcendentals=rows * hidden,
        ),
        name="rows",
    )(tokens, out_grad, router_weight, ids, w_gateup, w_down)


def per_device(tokens, out_grad, z_weight, router_weight, expert_ids, gate_up_weight, down_weight):
    flight = lax.axis_size("expert")
    w_gateup = gate_up_weight[0]
    xt, ht, pre_grad, dyk, score, logits, small, spot = expert_rows(
        flight, tokens, out_grad, router_weight, expert_ids, w_gateup, down_weight[0]
    )
    gate_up_grad, down_grad, router_grad, token_grad = reduce_grads(
        lax.axis_size("dp"),
        flight,
        xt,
        pre_grad,
        ht,
        dyk,
        score,
        w_gateup,
        tokens.T,
        router_weight,
        logits,
        small,
        expert_ids,
        spot,
        z_weight[:, None],
    )
    return (token_grad, router_grad, gate_up_grad, down_grad)


def solution(mesh):
    return jax.shard_map(
        per_device,
        mesh=mesh,
        in_specs=(
            P(("dp", "expert"), None),
            P(("dp", "expert"), None),
            P(("dp", "expert")),
            P(),
            P(("dp", "expert"), None),
            P("expert", None, None),
            P("expert", None, None),
        ),
        out_specs=(
            P(("dp", "expert"), None),
            P(),
            P("expert", "dp", None),
            P("expert", "dp", None),
        ),
        check_vma=False,
    )
```

```python
import functools

import jax
import jax.numpy as jnp
from jax import lax
from jax.experimental import pallas as pl
from jax.experimental.pallas import tpu as pltpu
from jax.sharding import PartitionSpec as P

F32 = jnp.float32
BF16 = jnp.bfloat16
MESH = pl.DeviceIdType.MESH


def ring_order(count):
    inner = max(k for k in range(1, count + 1) if count % k == 0 and k * k <= count)
    outer = count // inner
    if inner == 1 or outer % 2:
        return list(range(count))
    order = []
    for row in range(outer):
        cols = list(range(1, inner))
        order += [row * inner + col for col in (cols if row % 2 == 0 else cols[::-1])]
    return order + [row * inner for row in range(outer)][::-1]


def lookup(table, key):
    value = jnp.int32(0)
    for slot, entry in enumerate(table):
        value = value + jnp.where(key == slot, jnp.int32(entry), jnp.int32(0))
    return value


def grads_part(
    copies, flight, order, top,
    tok_ref, rw_ref, wg_ref, xt_ref, pg_ref, ht_ref, dy_ref, score_ref, logit_ref, small_ref, spot_ref, back, home_dx,
    gu_ref, dn_ref, rout_ref, tg_ref,
    gu_buf, dn_buf, rx_e, rsum, rx_d, rfull, rp_ref, home_score, lg_ref,
    send_sem, recv_sem, es_send, es_recv, ds_send, ds_recv, dg_send, dg_recv, eg_send, eg_recv,
    dx_send, dx_recv, sc_send, sc_recv,
):
    d = lax.axis_index("dp")
    e = lax.axis_index("expert")
    n = copies
    place = [order.index(i) for i in range(n)]
    pos = lookup(place, d)
    right = lookup(order, lax.rem(pos + 1, n))
    left = lookup(order, lax.rem(pos + n - 1, n))
    towards = (right, left)

    gu_rows = gu_ref.shape[1]
    half_rows = gu_rows // 2
    dn_rows = dn_ref.shape[1]
    gu_cols = gu_ref.shape[2] // 2
    dn_cols = dn_ref.shape[2] // 2
    piece_e = rsum.shape[0]
    piece_d = rx_d.shape[1]

    def owner_at(way, step):
        if way == 0:
            return lookup(order, lax.rem(pos + 2 * n - 1 - step, n))
        return lookup(order, lax.rem(pos + 1 + step, n))

    def own(way, part, owner):
        if part < 2:
            start = pl.multiple_of(owner * gu_rows + part * half_rows, half_rows)
            return jnp.dot(
                xt_ref[pl.ds(start, half_rows), :],
                pg_ref[:, way * gu_cols:(way + 1) * gu_cols],
                preferred_element_type=F32,
            )
        start = pl.multiple_of(owner * dn_rows, dn_rows)
        return jnp.dot(
            ht_ref[pl.ds(start, dn_rows), :],
            dy_ref[:, way * dn_cols:(way + 1) * dn_cols],
            preferred_element_type=F32,
        )

    def slot(way, part, step):
        return gu_buf.at[way, part, step] if part < 2 else dn_buf.at[way, step]

    def hop(way, part, step):
        return pltpu.make_async_remote_copy(
            src_ref=slot(way, part, step),
            dst_ref=slot(way, part, step + 1),
            send_sem=send_sem.at[way, part, step],
            recv_sem=recv_sem.at[way, part, step],
            device_id=(towards[way], e),
            device_id_type=MESH,
        )

    def share_e(k):
        to = lax.rem(e + k, flight)
        return pltpu.make_async_remote_copy(
            src_ref=rp_ref.at[pl.ds(pl.multiple_of(to * piece_e, piece_e), piece_e), :],
            dst_ref=rx_e.at[k - 1],
            send_sem=es_send.at[k - 1], recv_sem=es_recv.at[k - 1],
            device_id=(d, to), device_id_type=MESH,
        )

    def share_d(k):
        to = lax.rem(d + k, n)
        return pltpu.make_async_remote_copy(
            src_ref=rsum.at[pl.ds(pl.multiple_of(to * piece_d, piece_d), piece_d), :],
            dst_ref=rx_d.at[k - 1],
            send_sem=ds_send.at[k - 1], recv_sem=ds_recv.at[k - 1],
            device_id=(to, e), device_id_type=MESH,
        )

    def gather_d(k, source):
        rows = pl.ds(pl.multiple_of(e * piece_e + source * piece_d, piece_d), piece_d)
        return pltpu.make_async_remote_copy(
            src_ref=rfull.at[rows, :], dst_ref=rfull.at[rows, :],
            send_sem=dg_send.at[k - 1], recv_sem=dg_recv.at[k - 1],
            device_id=(lax.rem(d + k, n), e), device_id_type=MESH,
        )

    def gather_e(k, source):
        rows = pl.ds(pl.multiple_of(source * piece_e, piece_e), piece_e)
        return pltpu.make_async_remote_copy(
            src_ref=rfull.at[rows, :], dst_ref=rfull.at[rows, :],
            send_sem=eg_send.at[k - 1], recv_sem=eg_recv.at[k - 1],
            device_id=(d, lax.rem(e + k, flight)), device_id_type=MESH,
        )

    cap = home_score.shape[1]

    def block(ref, index):
        return ref.at[pl.ds(pl.multiple_of(index * cap, cap), cap), :]

    def give_score(k, source):
        to = lax.rem(e + k, flight)
        return pltpu.make_async_remote_copy(
            src_ref=block(score_ref, to), dst_ref=home_score.at[source],
            send_sem=sc_send.at[k - 1], recv_sem=sc_recv.at[k - 1],
            device_id=(d, to), device_id_type=MESH,
        )

    def give_dx(k, source):
        to = lax.rem(e + k, flight)
        return pltpu.make_async_remote_copy(
            src_ref=block(back, to), dst_ref=block(home_dx, source),
            send_sem=dx_send.at[k - 1], recv_sem=dx_recv.at[k - 1],
            device_id=(d, to), device_id_type=MESH,
        )

    def from_peer(k):
        return lax.rem(e + flight - k, flight)

    def one_hot(k):
        spots = lax.broadcasted_iota(jnp.int32, (tok_ref.shape[0], flight * cap), 1)
        return spots == spot_ref[:, k:k + 1]

    for part in range(3):
        for way in range(2):
            slot(way, part, 0)[...] = own(way, part, owner_at(way, 0)).astype(BF16)
            hop(way, part, 0).start()
    for k in range(1, flight):
        give_score(k, e).start()
    home_score[e] = score_ref[pl.ds(pl.multiple_of(e * cap, cap), cap), :]

    width = back.shape[1]
    tile = min(width, 512)
    for col in range(0, width, tile):
        back[:, col:col + tile] = lax.dot_general(
            pg_ref[...], wg_ref[col:col + tile, :], (((1,), (1,)), ((), ())),
            preferred_element_type=F32,
        ).astype(BF16)
    own_rows = pl.ds(pl.multiple_of(e * cap, cap), cap)
    home_dx[own_rows, :] = back[own_rows, :]

    def middle(step, carry):
        for part in range(3):
            for way in range(2):
                hop(way, part, step - 1).wait_recv()
                here = slot(way, part, step)
                here[...] = (
                    here[...].astype(F32) + own(way, part, owner_at(way, step))
                ).astype(BF16)
                hop(way, part, step).start()

        @pl.when(step == 1)
        def _():
            for k in range(1, flight):
                give_score(k, from_peer(k)).wait_recv()
            for k in range(1, flight):
                give_dx(k, e).start()
            arrived = home_score[...].reshape(flight * cap, home_score.shape[2])
            logits = logit_ref[...]
            lanes = lax.broadcasted_iota(jnp.int32, logits.shape, 1)
            scores = [
                jnp.dot(
                    one_hot(k).astype(F32), arrived,
                    precision=lax.Precision.HIGHEST, preferred_element_type=F32,
                )
                for k in range(top)
            ]
            probs = [small_ref[:, k:k + 1] for k in range(top)]
            mean = sum(p * q for p, q in zip(probs, scores))
            z_weight = small_ref[:, top + 1:top + 2]
            log_total = small_ref[:, top:top + 1]
            grad = 2.0 * z_weight * log_total * jnp.exp(logits - log_total)
            for k in range(top):
                grad = grad + jnp.where(
                    spot_ref[:, top + k:top + k + 1] == lanes, probs[k] * (scores[k] - mean), 0.0
                )
            lg_ref[...] = grad.astype(BF16)
            rp_ref[...] = jnp.dot(tok_ref[...].T, lg_ref[...], preferred_element_type=F32)
            for k in range(1, flight):
                share_e(k).start()

        @pl.when(step == 2)
        def _():
            total = rp_ref[pl.ds(pl.multiple_of(e * piece_e, piece_e), piece_e), :]
            for k in range(1, flight):
                share_e(k).wait_recv()
                total = total + rx_e[k - 1]
            rp_ref[pl.ds(pl.multiple_of(e * piece_e, piece_e), piece_e), :] = total
            rsum[...] = total.astype(BF16)
            for k in range(1, n):
                share_d(k).start()

        @pl.when(step == 3)
        def _():
            mine = pl.ds(pl.multiple_of(e * piece_e + d * piece_d, piece_d), piece_d)
            total = rp_ref[mine, :]
            for k in range(1, n):
                share_d(k).wait_recv()
                total = total + rx_d[k - 1].astype(F32)
            rfull[mine, :] = total
            for k in range(1, n):
                gather_d(k, d).start()

        @pl.when(step == 4)
        def _():
            for k in range(1, n):
                gather_d(k, lax.rem(d + n - k, n)).wait_recv()
            for k in range(1, flight):
                gather_e(k, e).start()

        @pl.when(step == 5)
        def _():
            for k in range(1, flight):
                give_dx(k, from_peer(k)).wait_recv()
            picks = sum(one_hot(k).astype(F32) for k in range(top)).astype(BF16)
            rows = home_dx[...]
            for col in range(0, width, tile):
                total = jnp.dot(picks, rows[:, col:col + tile], preferred_element_type=F32)
                total = total + lax.dot_general(
                    lg_ref[...], rw_ref[col:col + tile, :], (((1,), (1,)), ((), ())),
                    preferred_element_type=F32,
                )
                tg_ref[:, col:col + tile] = total.astype(BF16)

        return carry

    lax.fori_loop(1, n - 1, middle, 0)

    for k in range(1, flight):
        gather_e(k, from_peer(k)).wait_recv()
    rout_ref[...] = rfull[...]
    for part in range(3):
        for way in range(2):
            hop(way, part, n - 2).wait_recv()
            total = slot(way, part, n - 1)[...].astype(F32) + own(way, part, d)
            if part < 2:
                gu_ref[
                    0, part * half_rows:(part + 1) * half_rows, way * gu_cols:(way + 1) * gu_cols
                ] = total.astype(BF16)
            else:
                dn_ref[0, :, way * dn_cols:(way + 1) * dn_cols] = total.astype(BF16)

    def drain(step, carry):
        for part in range(3):
            for way in range(2):
                hop(way, part, step).wait_send()
        return carry

    lax.fori_loop(0, n - 1, drain, 0)
    for k in range(1, n):
        share_d(k).wait_send()
        gather_d(k, d).wait_send()
    for k in range(1, flight):
        share_e(k).wait_send()
        gather_e(k, e).wait_send()
        give_score(k, e).wait_send()
        give_dx(k, e).wait_send()


def rows_part(
    flight, cap,
    tok_ref, og_ref, rw_ref, ids_ref, zw_ref, load_g, load_d, greet,
    xt_ref, ht_ref, pg_ref, score_ref, logit_ref, small_ref, spot_ref,
    wg_ref, wd_ref, out_x, out_o, out_p, in_x, in_o, in_p, pre, hid,
    x_send, x_recv, o_send, o_recv, p_send, p_recv,
):
    d = lax.axis_index("dp")
    e = lax.axis_index("expert")
    top, tok_count = ids_ref.shape
    routed = rw_ref.shape[1]
    hidden_units, width = wd_ref.shape
    tile = min(hidden_units, 512)
    pairs = flight // 2
    lanes = lax.broadcasted_iota(jnp.int32, (tok_count, routed), 1)
    def column(row):
        return jnp.broadcast_to(row, (routed, tok_count)).T

    ids = [column(ids_ref[k:k + 1, :].astype(F32)).astype(jnp.int32) for k in range(top)]
    choose = [column_ids == lanes for column_ids in ids]
    member = sum(c.astype(F32) for c in choose)
    earlier = lax.broadcasted_iota(jnp.int32, (tok_count, tok_count), 0) > (
        lax.broadcasted_iota(jnp.int32, (tok_count, tok_count), 1)
    )
    rank = jnp.dot(earlier.astype(F32).astype(BF16), member.astype(BF16), preferred_element_type=F32)
    rank = jnp.where(member > 0.0, rank, -1.0)
    by_expert = rank.T.astype(jnp.int32)
    ranks = lax.broadcasted_iota(jnp.int32, (cap, tok_count), 0)
    picks = [by_expert[f:f + 1, :] == ranks for f in range(flight)]

    greet()

    def rows_of(index):
        return pl.ds(pl.multiple_of(index * cap, cap), cap)

    def peers():
        found = []
        for i in range(1, pairs):
            pair = lax.rem(lax.div(e, 2) + i, pairs)
            found += [pair * 2 + lax.rem(e, 2), pair * 2 + 1 - lax.rem(e, 2)]
        return found + [lax.div(e, 2) * 2 + 1 - lax.rem(e, 2)]

    def give(out, into, sends, recvs, source, target):
        return pltpu.make_async_remote_copy(
            src_ref=out.at[rows_of(target), :], dst_ref=into.at[rows_of(source), :],
            send_sem=sends.at[target], recv_sem=recvs.at[source],
            device_id=(d, target), device_id_type=MESH,
        )

    give_x = functools.partial(give, out_x, in_x, x_send, x_recv)
    give_o = functools.partial(give, out_o, in_o, o_send, o_recv)
    give_p = functools.partial(give, out_p, in_p, p_send, p_recv)

    for f in range(flight):
        out_x[f * cap:(f + 1) * cap, :] = jnp.dot(
            picks[f].astype(F32).astype(BF16), tok_ref[...], preferred_element_type=F32
        ).astype(BF16)
    for to in peers():
        give_x(e, to).start()
    for f in range(flight):
        out_o[f * cap:(f + 1) * cap, :] = jnp.dot(
            picks[f].astype(F32).astype(BF16), og_ref[...], preferred_element_type=F32
        ).astype(BF16)
    for to in peers():
        give_o(e, to).start()

    logits = jnp.dot(tok_ref[...], rw_ref[...], preferred_element_type=F32)
    logit_ref[...] = logits
    chosen = [
        jnp.exp(jnp.sum(jnp.where(c, logits, 0.0), axis=1, keepdims=True)) for c in choose
    ]
    norm = sum(chosen)
    probs = [c / norm for c in chosen]
    log_total = jnp.log(jnp.sum(jnp.exp(logits), axis=1, keepdims=True))
    small = jnp.where(lanes == top, log_total, column(zw_ref[...]))
    spot = jnp.full(lanes.shape, -1, jnp.int32)
    weight = jnp.zeros(lanes.shape, F32)
    place = jnp.where((rank >= 0.0) & (lanes < flight), rank + (lanes * cap).astype(F32) + 1.0, 0.0)
    for k in range(top):
        small = jnp.where(lanes == k, probs[k], small)
        at = jnp.sum(jnp.where(choose[k], place, 0.0), axis=1, keepdims=True) - 1.0
        spot = jnp.where(lanes == k, at.astype(jnp.int32), spot)
        spot = jnp.where(lanes == top + k, ids[k], spot)
        weight = weight + jnp.where(choose[k], probs[k], 0.0)
    small_ref[...] = small
    spot_ref[...] = spot
    weight = weight.T
    for f in range(flight):
        row = jnp.sum(jnp.where(picks[f], weight[f:f + 1, :], 0.0), axis=1, keepdims=True)
        out_p[f * cap:(f + 1) * cap, :] = jnp.broadcast_to(row, (cap, routed))
    for to in peers():
        give_p(e, to).start()
    in_x[rows_of(e), :] = out_x[rows_of(e), :]
    in_o[rows_of(e), :] = out_o[rows_of(e), :]
    in_p[rows_of(e), :] = out_p[rows_of(e), :]

    def arrived(gives, pair):
        for core in range(2):
            source = pair * 2 + core

            @pl.when(source != e)
            def _():
                for g in gives:
                    g(source, e).wait_recv()

    def pair_rows(pair):
        return pl.ds(pl.multiple_of(pair * (2 * cap), 2 * cap), 2 * cap)

    load_g.wait()
    load_d.wait()

    def one_pair(i, carry):
        pair = lax.rem(lax.div(e, 2) + i, pairs)
        rows = pair_rows(pair)
        arrived([give_x], pair)
        for col in range(0, 2 * hidden_units, tile):
            pre[:, col:col + tile] = jnp.dot(
                in_x[rows, :], wg_ref[:, col:col + tile], preferred_element_type=F32
            )
        xt_ref[:, rows] = in_x[rows, :].T
        arrived([give_o, give_p], pair)
        prob = in_p[rows, 0:1]
        score = jnp.zeros((2 * cap, 1), F32)
        for col in range(0, hidden_units, tile):
            raw = lax.dot_general(
                in_o[rows, :], wd_ref[col:col + tile, :], (((1,), (1,)), ((), ())),
                preferred_element_type=F32,
            )
            gate = pre[:, col:col + tile]
            up = pre[:, hidden_units + col:hidden_units + col + tile]
            sig = jax.nn.sigmoid(gate)
            active = gate * sig
            hidden = (active * up).astype(BF16)
            hid[:, col:col + tile] = hidden
            score = score + jnp.sum(raw * hidden.astype(F32), axis=1, keepdims=True)
            grad = prob * raw
            pg_ref[rows, col:col + tile] = (
                grad * up * sig * (1.0 + gate * (1.0 - sig))
            ).astype(BF16)
            pg_ref[rows, hidden_units + col:hidden_units + col + tile] = (grad * active).astype(BF16)
        score_ref[rows, :] = jnp.broadcast_to(score, (2 * cap, routed))
        in_o[rows, :] = (prob * in_o[rows, :].astype(F32)).astype(BF16)
        ht_ref[:, rows] = hid[...].T
        return carry

    lax.fori_loop(0, pairs, one_pair, 0)
    for to in peers():
        give_x(e, to).wait_send()
        give_o(e, to).wait_send()
        give_p(e, to).wait_send()


def layer_kernel(copies, flight, order, cap, *refs):
    tok_ref, og_ref, rw_ref, ids_ref, zw_ref, wg_hbm, wd_hbm = refs[:7]
    outs = refs[7:11]
    xt, ht, pg, score, logit, small, spot, wg_ref, wd_ref = refs[11:20]
    rows_scratch = refs[20:28]
    wg_sem, wd_sem = refs[28:30]
    rows_sems = refs[30:36]
    grads_scratch = refs[36:]
    out_x, in_x, dy = rows_scratch[0], rows_scratch[3], rows_scratch[4]
    d = lax.axis_index("dp")
    e = lax.axis_index("expert")
    load_g = pltpu.make_async_copy(wg_hbm, wg_ref, wg_sem)
    load_d = pltpu.make_async_copy(wd_hbm, wd_ref, wd_sem)
    load_g.start()
    load_d.start()
    barrier = pltpu.get_barrier_semaphore()
    for k in range(1, flight):
        to = lax.rem(e + k, flight)
        pl.semaphore_signal(barrier, inc=1, device_id=(d, to), device_id_type=MESH)
    for k in range(1, copies):
        to = lax.rem(d + k, copies)
        pl.semaphore_signal(barrier, inc=1, device_id=(to, e), device_id_type=MESH)

    def greet():
        pl.semaphore_wait(barrier, copies + flight - 2)

    rows_part(
        flight, cap, tok_ref, og_ref, rw_ref, ids_ref, zw_ref, load_g, load_d, greet,
        xt, ht, pg, score, logit, small, spot, wg_ref, wd_ref, *rows_scratch, *rows_sems,
    )
    grads_part(
        copies, flight, order, ids_ref.shape[0],
        tok_ref, rw_ref, wg_ref, xt, pg, ht, dy, score, logit, small, spot, out_x, in_x,
        *outs, *grads_scratch,
    )


def per_device(tokens, out_grad, z_weight, router_weight, expert_ids, gate_up_weight, down_weight):
    n = lax.axis_size("dp")
    flight = lax.axis_size("expert")
    w_gateup, w_down = gate_up_weight[0], down_weight[0]
    tok_count, width = tokens.shape
    routed = router_weight.shape[1]
    hidden = w_down.shape[0]
    gate_up = w_gateup.shape[1]
    cap = tok_count // 2
    rows = flight * cap
    gu_rows, dn_rows = width // n, hidden // n
    piece_e = width // flight
    piece_d = piece_e // n
    dma = pltpu.SemaphoreType.DMA
    vmem = pl.BlockSpec(memory_space=pltpu.VMEM)
    hbm = pl.BlockSpec(memory_space=pl.ANY)
    shape = jax.ShapeDtypeStruct
    gate_up_grad, down_grad, router_grad, token_grad = pl.pallas_call(
        functools.partial(layer_kernel, n, flight, ring_order(n), cap),
        out_shape=(
            shape((1, gu_rows, gate_up), BF16),
            shape((1, dn_rows, width), BF16),
            shape((width, routed), F32),
            shape((tok_count, width), BF16),
        ),
        in_specs=[vmem] * 5 + [hbm] * 2,
        out_specs=(vmem,) * 4,
        scratch_shapes=[
            pltpu.VMEM((width, rows), BF16),
            pltpu.VMEM((hidden, rows), BF16),
            pltpu.VMEM((rows, gate_up), BF16),
            pltpu.VMEM((rows, routed), F32),
            pltpu.VMEM((tok_count, routed), F32),
            pltpu.VMEM((tok_count, routed), F32),
            pltpu.VMEM((tok_count, routed), jnp.int32),
            pltpu.VMEM(w_gateup.shape, BF16),
            pltpu.VMEM(w_down.shape, BF16),
            pltpu.VMEM((rows, width), BF16),
            pltpu.VMEM((rows, width), BF16),
            pltpu.VMEM((rows, routed), F32),
            pltpu.VMEM((rows, width), BF16),
            pltpu.VMEM((rows, width), BF16),
            pltpu.VMEM((rows, routed), F32),
            pltpu.VMEM((2 * cap, gate_up), F32),
            pltpu.VMEM((2 * cap, hidden), BF16),
            dma, dma,
        ] + [dma((flight,))] * 6 + [
            pltpu.VMEM((2, 2, n, gu_rows // 2, gate_up // 2), BF16),
            pltpu.VMEM((2, n, dn_rows, width // 2), BF16),
            pltpu.VMEM((flight - 1, piece_e, routed), F32),
            pltpu.VMEM((piece_e, routed), BF16),
            pltpu.VMEM((n - 1, piece_d, routed), BF16),
            pltpu.VMEM((width, routed), F32),
            pltpu.VMEM((width, routed), F32),
            pltpu.VMEM((flight, cap, routed), F32),
            pltpu.VMEM((tok_count, routed), BF16),
            dma((2, 3, n - 1)), dma((2, 3, n - 1)),
            dma((flight - 1,)), dma((flight - 1,)),
            dma((n - 1,)), dma((n - 1,)),
            dma((n - 1,)), dma((n - 1,)),
            dma((flight - 1,)), dma((flight - 1,)),
            dma((flight - 1,)), dma((flight - 1,)),
            dma((flight - 1,)), dma((flight - 1,)),
        ],
        compiler_params=pltpu.CompilerParams(
            collective_id=0, has_side_effects=True, vmem_limit_bytes=67_000_000
        ),
        name="layer",
    )(
        tokens,
        out_grad,
        router_weight,
        expert_ids.T,
        z_weight[None, :],
        w_gateup,
        w_down,
    )
    return (token_grad, router_grad, gate_up_grad, down_grad)


def solution(mesh):
    return jax.shard_map(
        per_device,
        mesh=mesh,
        in_specs=(
            P(("dp", "expert"), None),
            P(("dp", "expert"), None),
            P(("dp", "expert")),
            P(),
            P(("dp", "expert"), None),
            P("expert", None, None),
            P("expert", None, None),
        ),
        out_specs=(
            P(("dp", "expert"), None),
            P(),
            P("expert", "dp", None),
            P("expert", "dp", None),
        ),
        check_vma=False,
    )
```

```python
import functools

import jax
import jax.numpy as jnp
from jax import lax
from jax.experimental import pallas as pl
from jax.experimental.pallas import tpu as pltpu
from jax.sharding import PartitionSpec as P

F32 = jnp.float32
BF16 = jnp.bfloat16
MESH = pl.DeviceIdType.MESH


def ring_order(count):
    inner = max(k for k in range(1, count + 1) if count % k == 0 and k * k <= count)
    outer = count // inner
    if inner == 1 or outer % 2:
        return list(range(count))
    order = []
    for row in range(outer):
        cols = list(range(1, inner))
        order += [row * inner + col for col in (cols if row % 2 == 0 else cols[::-1])]
    return order + [row * inner for row in range(outer)][::-1]


def lookup(table, key):
    value = jnp.int32(0)
    for slot, entry in enumerate(table):
        value = value + jnp.where(key == slot, jnp.int32(entry), jnp.int32(0))
    return value


def grads_part(
    copies, flight, order, top,
    tok_ref, rw_ref, wg_ref, xt_ref, pg_ref, ht_ref, dy_ref, score_ref, logit_ref, small_ref, spot_ref, back, home_dx,
    gu_ref, dn_ref, rout_ref, tg_ref,
    gu_buf, dn_buf, rx_e, rsum, rx_d, rfull, rp_ref, home_score, lg_ref,
    send_sem, recv_sem, es_send, es_recv, ds_send, ds_recv, dg_send, dg_recv, eg_send, eg_recv,
    dx_send, dx_recv, sc_send, sc_recv,
):
    d = lax.axis_index("dp")
    e = lax.axis_index("expert")
    n = copies
    place = [order.index(i) for i in range(n)]
    pos = lookup(place, d)
    right = lookup(order, lax.rem(pos + 1, n))
    left = lookup(order, lax.rem(pos + n - 1, n))
    towards = (right, left)

    gu_rows = gu_ref.shape[1]
    half_rows = gu_rows // 2
    dn_rows = dn_ref.shape[1]
    gu_cols = gu_ref.shape[2] // 2
    dn_cols = dn_ref.shape[2] // 2
    piece_e = rsum.shape[0]
    piece_d = rx_d.shape[1]

    def owner_at(way, step):
        if way == 0:
            return lookup(order, lax.rem(pos + 2 * n - 1 - step, n))
        return lookup(order, lax.rem(pos + 1 + step, n))

    def own(way, part, owner):
        if part < 2:
            start = pl.multiple_of(owner * gu_rows + part * half_rows, half_rows)
            return jnp.dot(
                xt_ref[pl.ds(start, half_rows), :],
                pg_ref[:, way * gu_cols:(way + 1) * gu_cols],
                preferred_element_type=F32,
            )
        start = pl.multiple_of(owner * dn_rows, dn_rows)
        return jnp.dot(
            ht_ref[pl.ds(start, dn_rows), :],
            dy_ref[:, way * dn_cols:(way + 1) * dn_cols],
            preferred_element_type=F32,
        )

    def slot(way, part, step):
        return gu_buf.at[way, part, step] if part < 2 else dn_buf.at[way, step]

    def hop(way, part, step):
        return pltpu.make_async_remote_copy(
            src_ref=slot(way, part, step),
            dst_ref=slot(way, part, step + 1),
            send_sem=send_sem.at[way, part, step],
            recv_sem=recv_sem.at[way, part, step],
            device_id=(towards[way], e),
            device_id_type=MESH,
        )

    def share_e(k):
        to = lax.rem(e + k, flight)
        return pltpu.make_async_remote_copy(
            src_ref=rp_ref.at[pl.ds(pl.multiple_of(to * piece_e, piece_e), piece_e), :],
            dst_ref=rx_e.at[k - 1],
            send_sem=es_send.at[k - 1], recv_sem=es_recv.at[k - 1],
            device_id=(d, to), device_id_type=MESH,
        )

    def share_d(k):
        to = lax.rem(d + k, n)
        return pltpu.make_async_remote_copy(
            src_ref=rsum.at[pl.ds(pl.multiple_of(to * piece_d, piece_d), piece_d), :],
            dst_ref=rx_d.at[k - 1],
            send_sem=ds_send.at[k - 1], recv_sem=ds_recv.at[k - 1],
            device_id=(to, e), device_id_type=MESH,
        )

    def gather_d(k, source):
        rows = pl.ds(pl.multiple_of(e * piece_e + source * piece_d, piece_d), piece_d)
        return pltpu.make_async_remote_copy(
            src_ref=rfull.at[rows, :], dst_ref=rfull.at[rows, :],
            send_sem=dg_send.at[k - 1], recv_sem=dg_recv.at[k - 1],
            device_id=(lax.rem(d + k, n), e), device_id_type=MESH,
        )

    def gather_e(k, source):
        rows = pl.ds(pl.multiple_of(source * piece_e, piece_e), piece_e)
        return pltpu.make_async_remote_copy(
            src_ref=rfull.at[rows, :], dst_ref=rfull.at[rows, :],
            send_sem=eg_send.at[k - 1], recv_sem=eg_recv.at[k - 1],
            device_id=(d, lax.rem(e + k, flight)), device_id_type=MESH,
        )

    cap = home_score.shape[1]

    def block(ref, index):
        return ref.at[pl.ds(pl.multiple_of(index * cap, cap), cap), :]

    def give_score(k, source):
        to = lax.rem(e + k, flight)
        return pltpu.make_async_remote_copy(
            src_ref=block(score_ref, to), dst_ref=home_score.at[source],
            send_sem=sc_send.at[k - 1], recv_sem=sc_recv.at[k - 1],
            device_id=(d, to), device_id_type=MESH,
        )

    def give_dx(k, source):
        to = lax.rem(e + k, flight)
        return pltpu.make_async_remote_copy(
            src_ref=block(back, to), dst_ref=block(home_dx, source),
            send_sem=dx_send.at[k - 1], recv_sem=dx_recv.at[k - 1],
            device_id=(d, to), device_id_type=MESH,
        )

    def from_peer(k):
        return lax.rem(e + flight - k, flight)

    def one_hot(k):
        spots = lax.broadcasted_iota(jnp.int32, (tok_ref.shape[0], flight * cap), 1)
        return spots == spot_ref[:, k:k + 1]

    for part in range(3):
        for way in range(2):
            slot(way, part, 0)[...] = own(way, part, owner_at(way, 0)).astype(BF16)
            hop(way, part, 0).start()
    for k in range(1, flight):
        give_score(k, e).start()
    home_score[e] = score_ref[pl.ds(pl.multiple_of(e * cap, cap), cap), :]

    width = back.shape[1]
    tile = min(width, 512)
    for col in range(0, width, tile):
        back[:, col:col + tile] = lax.dot_general(
            pg_ref[...], wg_ref[col:col + tile, :], (((1,), (1,)), ((), ())),
            preferred_element_type=F32,
        ).astype(BF16)
    own_rows = pl.ds(pl.multiple_of(e * cap, cap), cap)
    home_dx[own_rows, :] = back[own_rows, :]

    def middle(step, carry):
        for part in range(3):
            for way in range(2):
                hop(way, part, step - 1).wait_recv()
                here = slot(way, part, step)
                here[...] = (
                    here[...].astype(F32) + own(way, part, owner_at(way, step))
                ).astype(BF16)
                hop(way, part, step).start()

        @pl.when(step == 1)
        def _():
            for k in range(1, flight):
                give_score(k, from_peer(k)).wait_recv()
            for k in range(1, flight):
                give_dx(k, e).start()
            arrived = home_score[...].reshape(flight * cap, home_score.shape[2])
            logits = logit_ref[...]
            lanes = lax.broadcasted_iota(jnp.int32, logits.shape, 1)
            scores = [
                jnp.dot(
                    one_hot(k).astype(F32), arrived,
                    precision=lax.Precision.HIGHEST, preferred_element_type=F32,
                )
                for k in range(top)
            ]
            probs = [small_ref[:, k:k + 1] for k in range(top)]
            mean = sum(p * q for p, q in zip(probs, scores))
            z_weight = small_ref[:, top + 1:top + 2]
            log_total = small_ref[:, top:top + 1]
            grad = 2.0 * z_weight * log_total * jnp.exp(logits - log_total)
            for k in range(top):
                grad = grad + jnp.where(
                    spot_ref[:, top + k:top + k + 1] == lanes, probs[k] * (scores[k] - mean), 0.0
                )
            lg_ref[...] = grad.astype(BF16)
            rp_ref[...] = jnp.dot(tok_ref[...].T, lg_ref[...], preferred_element_type=F32)
            for k in range(1, flight):
                share_e(k).start()

        @pl.when(step == 2)
        def _():
            total = rp_ref[pl.ds(pl.multiple_of(e * piece_e, piece_e), piece_e), :]
            for k in range(1, flight):
                share_e(k).wait_recv()
                total = total + rx_e[k - 1]
            rp_ref[pl.ds(pl.multiple_of(e * piece_e, piece_e), piece_e), :] = total
            rsum[...] = total.astype(BF16)
            for k in range(1, n):
                share_d(k).start()

        @pl.when(step == 3)
        def _():
            mine = pl.ds(pl.multiple_of(e * piece_e + d * piece_d, piece_d), piece_d)
            total = rp_ref[mine, :]
            for k in range(1, n):
                share_d(k).wait_recv()
                total = total + rx_d[k - 1].astype(F32)
            rfull[mine, :] = total
            for k in range(1, n):
                gather_d(k, d).start()

        @pl.when(step == 4)
        def _():
            for k in range(1, n):
                gather_d(k, lax.rem(d + n - k, n)).wait_recv()
            for k in range(1, flight):
                gather_e(k, e).start()

        @pl.when(step == 5)
        def _():
            for k in range(1, flight):
                give_dx(k, from_peer(k)).wait_recv()
            picks = sum(one_hot(k).astype(F32) for k in range(top)).astype(BF16)
            rows = home_dx[...]
            for col in range(0, width, tile):
                total = jnp.dot(picks, rows[:, col:col + tile], preferred_element_type=F32)
                total = total + lax.dot_general(
                    lg_ref[...], rw_ref[col:col + tile, :], (((1,), (1,)), ((), ())),
                    preferred_element_type=F32,
                )
                tg_ref[:, col:col + tile] = total.astype(BF16)

        return carry

    lax.fori_loop(1, n - 1, middle, 0)

    for k in range(1, flight):
        gather_e(k, from_peer(k)).wait_recv()
    rout_ref[...] = rfull[...]
    for part in range(3):
        for way in range(2):
            hop(way, part, n - 2).wait_recv()
            total = slot(way, part, n - 1)[...].astype(F32) + own(way, part, d)
            if part < 2:
                gu_ref[
                    0, part * half_rows:(part + 1) * half_rows, way * gu_cols:(way + 1) * gu_cols
                ] = total.astype(BF16)
            else:
                dn_ref[0, :, way * dn_cols:(way + 1) * dn_cols] = total.astype(BF16)

    def drain(step, carry):
        for part in range(3):
            for way in range(2):
                hop(way, part, step).wait_send()
        return carry

    lax.fori_loop(0, n - 1, drain, 0)
    for k in range(1, n):
        share_d(k).wait_send()
        gather_d(k, d).wait_send()
    for k in range(1, flight):
        share_e(k).wait_send()
        gather_e(k, e).wait_send()
        give_score(k, e).wait_send()
        give_dx(k, e).wait_send()


def rows_part(
    flight, cap,
    tok_ref, og_ref, rw_ref, ids_ref, zw_ref, load_g, load_d, greet,
    xt_ref, ht_ref, pg_ref, score_ref, logit_ref, small_ref, spot_ref,
    wg_ref, wd_ref, out_x, out_o, out_p, in_x, in_o, in_p, pre, hid,
    x_send, x_recv, o_send, o_recv, p_send, p_recv,
):
    d = lax.axis_index("dp")
    e = lax.axis_index("expert")
    top, tok_count = ids_ref.shape
    routed = rw_ref.shape[1]
    hidden_units, width = wd_ref.shape
    tile = min(hidden_units, 512)
    pairs = flight // 2
    lanes = lax.broadcasted_iota(jnp.int32, (tok_count, routed), 1)
    def column(row):
        return jnp.broadcast_to(row, (routed, tok_count)).T

    ids = [column(ids_ref[k:k + 1, :].astype(F32)).astype(jnp.int32) for k in range(top)]
    choose = [column_ids == lanes for column_ids in ids]
    member = sum(c.astype(F32) for c in choose)
    earlier = lax.broadcasted_iota(jnp.int32, (tok_count, tok_count), 0) > (
        lax.broadcasted_iota(jnp.int32, (tok_count, tok_count), 1)
    )
    rank = jnp.dot(earlier.astype(F32).astype(BF16), member.astype(BF16), preferred_element_type=F32)
    rank = jnp.where(member > 0.0, rank, -1.0)
    by_expert = rank.T.astype(jnp.int32)
    ranks = lax.broadcasted_iota(jnp.int32, (cap, tok_count), 0)
    picks = [by_expert[f:f + 1, :] == ranks for f in range(flight)]

    greet()

    def rows_of(index):
        return pl.ds(pl.multiple_of(index * cap, cap), cap)

    def peers():
        found = []
        for i in range(1, pairs):
            pair = lax.rem(lax.div(e, 2) + i, pairs)
            found += [pair * 2 + lax.rem(e, 2), pair * 2 + 1 - lax.rem(e, 2)]
        return found + [lax.div(e, 2) * 2 + 1 - lax.rem(e, 2)]

    def give(out, into, sends, recvs, source, target):
        return pltpu.make_async_remote_copy(
            src_ref=out.at[rows_of(target), :], dst_ref=into.at[rows_of(source), :],
            send_sem=sends.at[target], recv_sem=recvs.at[source],
            device_id=(d, target), device_id_type=MESH,
        )

    give_x = functools.partial(give, out_x, in_x, x_send, x_recv)
    give_o = functools.partial(give, out_o, in_o, o_send, o_recv)
    give_p = functools.partial(give, out_p, in_p, p_send, p_recv)

    for f in range(flight):
        out_x[f * cap:(f + 1) * cap, :] = jnp.dot(
            picks[f].astype(F32).astype(BF16), tok_ref[...], preferred_element_type=F32
        ).astype(BF16)
    for to in peers():
        give_x(e, to).start()
    for f in range(flight):
        out_o[f * cap:(f + 1) * cap, :] = jnp.dot(
            picks[f].astype(F32).astype(BF16), og_ref[...], preferred_element_type=F32
        ).astype(BF16)
    for to in peers():
        give_o(e, to).start()

    logits = jnp.dot(tok_ref[...], rw_ref[...], preferred_element_type=F32)
    logit_ref[...] = logits
    chosen = [
        jnp.exp(jnp.sum(jnp.where(c, logits, 0.0), axis=1, keepdims=True)) for c in choose
    ]
    norm = sum(chosen)
    probs = [c / norm for c in chosen]
    log_total = jnp.log(jnp.sum(jnp.exp(logits), axis=1, keepdims=True))
    small = jnp.where(lanes == top, log_total, column(zw_ref[...]))
    spot = jnp.full(lanes.shape, -1, jnp.int32)
    weight = jnp.zeros(lanes.shape, F32)
    place = jnp.where((rank >= 0.0) & (lanes < flight), rank + (lanes * cap).astype(F32) + 1.0, 0.0)
    for k in range(top):
        small = jnp.where(lanes == k, probs[k], small)
        at = jnp.sum(jnp.where(choose[k], place, 0.0), axis=1, keepdims=True) - 1.0
        spot = jnp.where(lanes == k, at.astype(jnp.int32), spot)
        spot = jnp.where(lanes == top + k, ids[k], spot)
        weight = weight + jnp.where(choose[k], probs[k], 0.0)
    small_ref[...] = small
    spot_ref[...] = spot
    weight = weight.T
    for f in range(flight):
        row = jnp.sum(jnp.where(picks[f], weight[f:f + 1, :], 0.0), axis=1, keepdims=True)
        out_p[f * cap:(f + 1) * cap, :] = jnp.broadcast_to(row, (cap, routed))
    for to in peers():
        give_p(e, to).start()
    in_x[rows_of(e), :] = out_x[rows_of(e), :]
    in_o[rows_of(e), :] = out_o[rows_of(e), :]
    in_p[rows_of(e), :] = out_p[rows_of(e), :]

    def arrived(gives, pair):
        for core in range(2):
            source = pair * 2 + core

            @pl.when(source != e)
            def _():
                for g in gives:
                    g(source, e).wait_recv()

    def pair_rows(pair):
        return pl.ds(pl.multiple_of(pair * (2 * cap), 2 * cap), 2 * cap)

    load_g.wait()
    load_d.wait()

    def one_pair(i, carry):
        pair = lax.rem(lax.div(e, 2) + i, pairs)
        rows = pair_rows(pair)
        arrived([give_x], pair)
        for col in range(0, 2 * hidden_units, tile):
            pre[:, col:col + tile] = jnp.dot(
                in_x[rows, :], wg_ref[:, col:col + tile], preferred_element_type=F32
            )
        xt_ref[:, rows] = in_x[rows, :].T
        arrived([give_o, give_p], pair)
        prob = in_p[rows, 0:1]
        score = jnp.zeros((2 * cap, 1), F32)
        for col in range(0, hidden_units, tile):
            raw = lax.dot_general(
                in_o[rows, :], wd_ref[col:col + tile, :], (((1,), (1,)), ((), ())),
                preferred_element_type=F32,
            )
            gate = pre[:, col:col + tile]
            up = pre[:, hidden_units + col:hidden_units + col + tile]
            sig = jax.nn.sigmoid(gate)
            active = gate * sig
            hidden = (active * up).astype(BF16)
            hid[:, col:col + tile] = hidden
            score = score + jnp.sum(raw * hidden.astype(F32), axis=1, keepdims=True)
            grad = prob * raw
            pg_ref[rows, col:col + tile] = (
                grad * up * sig * (1.0 + gate * (1.0 - sig))
            ).astype(BF16)
            pg_ref[rows, hidden_units + col:hidden_units + col + tile] = (grad * active).astype(BF16)
        score_ref[rows, :] = jnp.broadcast_to(score, (2 * cap, routed))
        in_o[rows, :] = (prob * in_o[rows, :].astype(F32)).astype(BF16)
        ht_ref[:, rows] = hid[...].T
        return carry

    lax.fori_loop(0, pairs, one_pair, 0)
    for to in peers():
        give_x(e, to).wait_send()
        give_o(e, to).wait_send()
        give_p(e, to).wait_send()


def layer_kernel(copies, flight, order, cap, *refs):
    tok_ref, og_ref, rw_ref, ids_ref, zw_ref, wg_hbm, wd_hbm = refs[:7]
    outs = refs[7:11]
    xt, ht, pg, score, logit, small, spot, wg_ref, wd_ref = refs[11:20]
    rows_scratch = refs[20:28]
    wg_sem, wd_sem = refs[28:30]
    rows_sems = refs[30:36]
    grads_scratch = refs[36:]
    out_x, in_x, dy = rows_scratch[0], rows_scratch[3], rows_scratch[4]
    d = lax.axis_index("dp")
    e = lax.axis_index("expert")
    load_g = pltpu.make_async_copy(wg_hbm, wg_ref, wg_sem)
    load_d = pltpu.make_async_copy(wd_hbm, wd_ref, wd_sem)
    load_g.start()
    load_d.start()
    barrier = pltpu.get_barrier_semaphore()
    for k in range(1, flight):
        to = lax.rem(e + k, flight)
        pl.semaphore_signal(barrier, inc=1, device_id=(d, to), device_id_type=MESH)
    for k in range(1, copies):
        to = lax.rem(d + k, copies)
        pl.semaphore_signal(barrier, inc=1, device_id=(to, e), device_id_type=MESH)

    def greet():
        pl.semaphore_wait(barrier, copies + flight - 2)

    rows_part(
        flight, cap, tok_ref, og_ref, rw_ref, ids_ref, zw_ref, load_g, load_d, greet,
        xt, ht, pg, score, logit, small, spot, wg_ref, wd_ref, *rows_scratch, *rows_sems,
    )
    grads_part(
        copies, flight, order, ids_ref.shape[0],
        tok_ref, rw_ref, wg_ref, xt, pg, ht, dy, score, logit, small, spot, out_x, in_x,
        *outs, *grads_scratch,
    )


def finish_kernel(*refs):
    for source, target in zip(refs[:4], refs[4:]):
        target[...] = source[...]


def per_device(tokens, out_grad, z_weight, router_weight, expert_ids, gate_up_weight, down_weight):
    n = lax.axis_size("dp")
    flight = lax.axis_size("expert")
    w_gateup, w_down = gate_up_weight[0], down_weight[0]
    tok_count, width = tokens.shape
    routed = router_weight.shape[1]
    hidden = w_down.shape[0]
    gate_up = w_gateup.shape[1]
    cap = tok_count // 2
    rows = flight * cap
    gu_rows, dn_rows = width // n, hidden // n
    piece_e = width // flight
    piece_d = piece_e // n
    dma = pltpu.SemaphoreType.DMA
    vmem = pl.BlockSpec(memory_space=pltpu.VMEM)
    hbm = pl.BlockSpec(memory_space=pl.ANY)
    shape = jax.ShapeDtypeStruct
    gate_up_grad, down_grad, router_grad, token_grad = pl.pallas_call(
        functools.partial(layer_kernel, n, flight, ring_order(n), cap),
        out_shape=(
            shape((1, gu_rows, gate_up), BF16),
            shape((1, dn_rows, width), BF16),
            shape((width, routed), F32),
            shape((tok_count, width), BF16),
        ),
        in_specs=[vmem] * 5 + [hbm] * 2,
        out_specs=(vmem,) * 4,
        scratch_shapes=[
            pltpu.VMEM((width, rows), BF16),
            pltpu.VMEM((hidden, rows), BF16),
            pltpu.VMEM((rows, gate_up), BF16),
            pltpu.VMEM((rows, routed), F32),
            pltpu.VMEM((tok_count, routed), F32),
            pltpu.VMEM((tok_count, routed), F32),
            pltpu.VMEM((tok_count, routed), jnp.int32),
            pltpu.VMEM(w_gateup.shape, BF16),
            pltpu.VMEM(w_down.shape, BF16),
            pltpu.VMEM((rows, width), BF16),
            pltpu.VMEM((rows, width), BF16),
            pltpu.VMEM((rows, routed), F32),
            pltpu.VMEM((rows, width), BF16),
            pltpu.VMEM((rows, width), BF16),
            pltpu.VMEM((rows, routed), F32),
            pltpu.VMEM((2 * cap, gate_up), F32),
            pltpu.VMEM((2 * cap, hidden), BF16),
            dma, dma,
        ] + [dma((flight,))] * 6 + [
            pltpu.VMEM((2, 2, n, gu_rows // 2, gate_up // 2), BF16),
            pltpu.VMEM((2, n, dn_rows, width // 2), BF16),
            pltpu.VMEM((flight - 1, piece_e, routed), F32),
            pltpu.VMEM((piece_e, routed), BF16),
            pltpu.VMEM((n - 1, piece_d, routed), BF16),
            pltpu.VMEM((width, routed), F32),
            pltpu.VMEM((width, routed), F32),
            pltpu.VMEM((flight, cap, routed), F32),
            pltpu.VMEM((tok_count, routed), BF16),
            dma((2, 3, n - 1)), dma((2, 3, n - 1)),
            dma((flight - 1,)), dma((flight - 1,)),
            dma((n - 1,)), dma((n - 1,)),
            dma((n - 1,)), dma((n - 1,)),
            dma((flight - 1,)), dma((flight - 1,)),
            dma((flight - 1,)), dma((flight - 1,)),
            dma((flight - 1,)), dma((flight - 1,)),
        ],
        compiler_params=pltpu.CompilerParams(
            collective_id=0, has_side_effects=True, vmem_limit_bytes=67_000_000
        ),
        name="layer",
    )(
        tokens,
        out_grad,
        router_weight,
        expert_ids.T,
        z_weight[None, :],
        w_gateup,
        w_down,
    )
    results = (token_grad, router_grad, gate_up_grad, down_grad)
    return pl.pallas_call(
        finish_kernel,
        out_shape=tuple(shape(r.shape, r.dtype) for r in results),
        in_specs=[vmem] * 4,
        out_specs=(vmem,) * 4,
        compiler_params=pltpu.CompilerParams(vmem_limit_bytes=16 * 2**20),
        name="finish",
    )(*results)


def solution(mesh):
    return jax.shard_map(
        per_device,
        mesh=mesh,
        in_specs=(
            P(("dp", "expert"), None),
            P(("dp", "expert"), None),
            P(("dp", "expert")),
            P(),
            P(("dp", "expert"), None),
            P("expert", None, None),
            P("expert", None, None),
        ),
        out_specs=(
            P(("dp", "expert"), None),
            P(),
            P("expert", "dp", None),
            P("expert", "dp", None),
        ),
        check_vma=False,
    )
```
